32 devices in a mesh: grp: 4 (over y, x), row: 8 (over z, core).
Axes of the slice: x: 2, y: 2, z: 4, core: 2. Of those that a mesh axis runs over, the one named last changes fastest.
Arguments:
- krylov_basis: bfloat16 [300, 512, 512], P(None, 'row', 'grp'), may hold values from -30 to 30
- krylov_image: bfloat16 [300, 512, 512], P(None, 'row', 'grp'), may hold values from -30 to 30
- tridiag_vectors: bfloat16 [300, 32], P(None, 'grp'), may hold values from -0.375 to 0.375
- ritz_values: bfloat16 [32], P('grp'), may hold values from -3 to 3
Outputs:
- ritz_vectors: float32 [32, 512, 512], P('grp', 'row')
- ritz_residuals: float32 [32, 512, 512], P('grp', 'row')
- residual_norms: float32 [32], P('grp')
The draws below stay inside these ranges and needn't reach their ends.
All inputs are finite; a program needn't handle non-finite values.
Results may differ from the reference program's by a relative error of at most 0.0003.
Values may be sent and summed in bfloat16 or wider, within the bound.
A program may use at most 64 MiB of HBM per device.

```python
import jax
import jax.numpy as jnp
from jax import lax

KRYLOV = 300
WANTED = 32
OUTER_DEV = 64
INNER_DEV = 128
OUTER = 512
INNER = 512
ROWS = 262144


def block_field(key):
    key_noise, key_scale, key_coef, key_common = jax.random.split(key, 4)
    blocks_outer = OUTER // OUTER_DEV
    blocks_inner = INNER // INNER_DEV
    noise_field = jax.random.normal(key_noise, (KRYLOV, OUTER, INNER), jnp.float32)
    levels = jax.random.uniform(key_scale, (blocks_outer, blocks_inner), jnp.float32, -0.7, 0.7)
    scales = jnp.exp(levels)
    scales = jnp.repeat(jnp.repeat(scales, OUTER_DEV, axis=0), INNER_DEV, axis=1)
    values_field = noise_field * scales[None, :, :]
    return jnp.clip(values_field, -30.0, 30.0).astype(jnp.bfloat16)


def draw_krylov_basis(key, part):
    return block_field(jax.random.fold_in(key, 11))


def draw_krylov_image(key, part):
    return block_field(jax.random.fold_in(key, 23))


def shard_levels(key, extent, pieces, least, high):
    factor_of, own = 1.0, jax.random.fold_in(key, 6)
    for dim, blocks in pieces:
        steps = jnp.exp(jax.random.uniform(jax.random.fold_in(own, dim), (blocks,), jnp.float32, least / len(pieces), high / len(pieces)))
        factor_of = factor_of * jnp.repeat(steps, extent[dim] // blocks).reshape([-1 if axis == dim else 1 for axis in range(len(extent))])
    return factor_of


def noise(rng, shape, width, bound, cuts=(), dtype=jnp.bfloat16):
    drawn = jax.random.normal(rng, shape, jnp.float32) * width
    if len(cuts) > 0:
        drawn = shard_levels(rng, shape, cuts, -0.22, 0.18) * drawn
    return jnp.clip(drawn, min=-bound, max=bound).astype(dtype)


def setup_inputs(seed: int = 0) -> dict:
    key_of = jax.random.split(jax.random.key(seed), 5)
    return {
        "krylov_basis": draw_krylov_basis(jax.random.fold_in(key_of[4], 71), 0),
        "krylov_image": draw_krylov_image(jax.random.fold_in(key_of[4], 71), 0),
        "tridiag_vectors": noise(key_of[2], (KRYLOV, WANTED), KRYLOV ** -0.5, 0.375, ((1, 4),)),
        "ritz_values": jnp.clip(jax.random.uniform(key_of[3], (WANTED,), jnp.float32, -3.0, 3.0) * shard_levels(key_of[3], (WANTED,), ((0, 4),), -0.4, 0.0), -3.0, 3.0).astype(jnp.bfloat16),
    }


def reference(krylov_basis, krylov_image, tridiag_vectors, ritz_values):
    flat_basis = krylov_basis.reshape(KRYLOV, OUTER * INNER)
    flat_image = krylov_image.reshape(KRYLOV, OUTER * INNER)
    coef_rows = tridiag_vectors.T
    ritz_cols = jnp.dot(coef_rows, flat_basis, preferred_element_type=jnp.float32)
    applied = jnp.dot(coef_rows, flat_image, preferred_element_type=jnp.float32)
    shift_values = ritz_values.astype(jnp.float32)
    resid_cols = applied - shift_values[:, None] * ritz_cols
    ritz_squares = lax.optimization_barrier(jnp.sum(ritz_cols * ritz_cols, axis=1)) + 1.0
    resid_squares = lax.optimization_barrier(jnp.sum(resid_cols * resid_cols, axis=1))
    factor = jnp.sqrt(ROWS / ritz_squares)
    ritz_vectors = (ritz_cols * factor[:, None]).reshape(WANTED, OUTER, INNER)
    ritz_residuals = (resid_cols * factor[:, None]).reshape(WANTED, OUTER, INNER)
    residual_norms = jnp.sqrt(resid_squares / ritz_squares)
    return (ritz_vectors, ritz_residuals, residual_norms)
```

```python
import functools
import math

import jax
import jax.numpy as jnp
from jax import lax
from jax.experimental import pallas as pl
from jax.experimental.pallas import tpu as pltpu
from jax.sharding import PartitionSpec as P

MESH = pl.DeviceIdType.MESH
MIB = 1 << 20
TILE = 8
STEP = 16
LANES = 128
POWER = 13
PEAK = 2.0 ** (126.0 / POWER)
SHIFT = 2.0**30
LEAST = 1e-36


def cdiv(a, b):
    return (a + b - 1) // b


def grid_iota(shape, dim):
    return lax.broadcasted_iota(jnp.int32, shape, dim)


def expand_rows(cols, width):
    return jnp.broadcast_to(cols, (cols.shape[0], width)).reshape(cols.shape[0], 1, width)


def encode(cols, inverse):
    y = cols * inverse
    y2 = y * y
    y4 = y2 * y2
    y8 = y4 * y4
    return (y8 * y4) * y


def decode(codes):
    size = jnp.exp2(jnp.log(jnp.abs(codes)) * (1.0 / (POWER * math.log(2.0))))
    return jnp.where(codes < 0.0, -size, size)


def exchange_kernel(
    groups, rows,
    tridiag_ref, values_ref, basis_ref, image_ref,
    ritz_ref, resid_ref, total_ref,
    coefs, values, fields, spread, reps, expanded, coded, received,
    stat_send, stat_recv, square_send, square_recv,
    coef_load, coef_send, coef_recv, load_sem, data_sems, stat_sems, square_sems,
    ready_sem, plane_sem, go_sem,
):
    wanted_dev, krylov_len = tridiag_ref.shape
    chunks = fields.shape[1]
    padded_len = fields.shape[2]
    inner_dev = basis_ref.shape[2]
    steps = padded_len // STEP
    wide = STEP * TILE
    block = wanted_dev * TILE
    planes = rows // 2
    grp = lax.axis_index("grp")
    row = lax.axis_index("row")
    core = lax.rem(row, 2)
    plane = lax.div(row, 2)
    lead = core == 1

    def partner(mask):
        if mask == 0:
            return grp
        if mask == 1:
            return grp + 1 - 2 * lax.rem(grp, 2)
        if mask == 2:
            return lax.rem(grp + 2, groups)
        return groups - 1 - grp

    def device(mask, at_plane, at_core):
        return {"grp": partner(mask), "row": 2 * at_plane + at_core}

    def signal(sem, where):
        pl.semaphore_signal(sem, inc=1, device_id=where, device_id_type=MESH)

    barrier = pltpu.get_barrier_semaphore()
    for mask in (1, 2):
        signal(barrier, device(mask, plane, 1))

    coef_loads = [
        pltpu.make_async_copy(tridiag_ref, coefs.at[0], coef_load.at[0]),
        pltpu.make_async_copy(values_ref, values.at[0], coef_load.at[1]),
    ]
    for copy in coef_loads:
        copy.start()

    @pl.when(core == 0)
    def _():
        signal(barrier, device(0, plane, 1))

        def greet(ahead, carry):
            signal(barrier, device(0, lax.rem(plane + ahead, planes), 0))
            return carry

        lax.fori_loop(1, planes, greet, 0)

    def loads(chunk):
        span = pl.ds(pl.multiple_of(chunk * TILE, TILE), TILE)
        return [
            pltpu.make_async_copy(
                ref.at[:, span, :], fields.at[which, chunk, pl.ds(0, krylov_len)], load_sem.at[which, chunk]
            )
            for which, ref in enumerate((basis_ref, image_ref))
        ]

    for chunk in range(chunks):
        for copy in loads(chunk):
            copy.start()

    if padded_len > krylov_len:
        for chunk in range(chunks):
            for which in range(2):
                fields[which, chunk, pl.ds(krylov_len, padded_len - krylov_len)] = jnp.zeros(
                    (padded_len - krylov_len, TILE, inner_dev), jnp.bfloat16
                )
    shape = spread.shape
    spread[...] = jnp.where(
        lax.shift_right_logical(grid_iota(shape, 1), 3) == grid_iota(shape, 0), SHIFT, 0.0
    ).astype(jnp.bfloat16)

    for copy in coef_loads:
        copy.wait()

    def coef_copies(source, slot, number, mask, at_core):
        return [
            pltpu.make_async_remote_copy(
                src_ref=ref.at[source],
                dst_ref=ref.at[slot],
                send_sem=coef_send.at[number, kind],
                recv_sem=coef_recv.at[slot - 1, kind],
                device_id=device(mask, plane, at_core),
                device_id_type=MESH,
            )
            for kind, ref in enumerate((coefs, values))
        ]

    own_sends = [
        copy
        for mask in (1, 2)
        for at_core in (1, 0)
        for copy in coef_copies(0, mask, 2 * mask + at_core - 2, mask, at_core)
    ]
    relay_sends = [copy for at_core in (1, 0) for copy in coef_copies(1, 3, 4 + at_core, 2, at_core)]

    def coef_wait(slot):
        for copy in coef_copies(0, slot, 0, 1, 1):
            copy.wait_recv()

    @pl.when(lead)
    def _():
        pl.semaphore_wait(barrier, 5)
        for copy in own_sends:
            copy.start()
        signal(ready_sem, device(0, plane, 0))
        coef_wait(1)
        for copy in relay_sends:
            copy.start()
        coef_wait(2)

    @pl.when(core == 0)
    def _():
        pl.semaphore_wait(ready_sem, 1)
        coef_wait(1)
        coef_wait(2)

    near = grid_iota((wanted_dev, wanted_dev), 0) == grid_iota((wanted_dev, wanted_dev), 1)
    same = (grid_iota((TILE, wide), 1) & (TILE - 1)) == grid_iota((TILE, wide), 0)
    per_part = LANES // STEP
    pair = 2 * wanted_dev
    lane = grid_iota((pair, LANES), 1)

    def prepare(slots):
        shifts = []
        for slot in slots:
            spot = jnp.broadcast_to(values[slot].astype(jnp.float32), (wanted_dev, wanted_dev))
            shifts.append(jnp.sum(jnp.where(near, spot, 0.0), axis=1, keepdims=True))
        shift_values = expand_rows(jnp.concatenate(shifts, axis=0), inner_dev)
        both = jnp.concatenate([coefs[slot] for slot in slots], axis=0)
        for part in range(cdiv(krylov_len, LANES)):
            piece = both[:, part * LANES : min((part + 1) * LANES, krylov_len)]
            reps[part] = jnp.dot(piece, spread[: piece.shape[1]], preferred_element_type=jnp.float32)
        for step in range(steps):
            at = (step % per_part) * wide
            spot = reps[step // per_part, :, at : at + wide]
            spot = jnp.where(same[None], spot.reshape(pair, 1, wide), 0.0)
            expanded[:, step * wide : (step + 1) * wide] = spot.reshape(pair * TILE, wide).astype(jnp.bfloat16)
        return shift_values

    def compute(slots, shift_values, chunk, stats):
        both = jnp.concatenate(
            [fields[which, chunk].reshape(padded_len * TILE, inner_dev) for which in range(2)], axis=1
        )
        product = jnp.dot(expanded[...], both, preferred_element_type=jnp.float32)
        product = product.reshape(pair, TILE, 2 * inner_dev)
        ritz = product[:, :, :inner_dev]
        resid = product[:, :, inner_dev:] - shift_values * ritz
        for kind, cols in enumerate((ritz, resid)):
            squares = jnp.sum(jnp.sum(cols * cols, axis=1), axis=1, keepdims=True)
            stats = jnp.where(lane == 2 * chunk + kind, squares, stats)
            inverse = expand_rows(PEAK / jnp.sqrt(jnp.maximum(squares, LEAST)), inner_dev)
            for index, slot in enumerate(slots):
                part = slice(index * wanted_dev, (index + 1) * wanted_dev)
                if slot == 0:
                    put_out(kind, chunk, grp, cols[part])
                else:
                    coded[slot - 1, chunk, :, kind * inner_dev : (kind + 1) * inner_dev] = encode(
                        cols[part], inverse[part]
                    ).reshape(block, inner_dev).astype(jnp.bfloat16)
        return stats

    def put_out(kind, chunk, source, cols):
        span = pl.ds(pl.multiple_of(chunk * TILE, TILE), TILE)
        lanes = pl.ds(pl.multiple_of(source * inner_dev, inner_dev), inner_dev)
        (ritz_ref, resid_ref)[kind][:, span, lanes] = cols

    def data_copy(mask, chunk):
        return pltpu.make_async_remote_copy(
            src_ref=coded.at[mask - 1, chunk],
            dst_ref=received.at[mask - 1, chunk],
            send_sem=data_sems.at[0, mask - 1, chunk],
            recv_sem=data_sems.at[1, mask - 1, chunk],
            device_id=device(mask, plane, core),
            device_id_type=MESH,
        )

    def stat_copy(mask):
        return pltpu.make_async_remote_copy(
            src_ref=stat_send.at[mask],
            dst_ref=stat_recv.at[mask],
            send_sem=stat_sems.at[0, mask],
            recv_sem=stat_sems.at[1, mask],
            device_id=device(mask, plane, core),
            device_id_type=MESH,
        )

    def square_copy(mask, ahead, flip):
        return pltpu.make_async_remote_copy(
            src_ref=square_send.at[mask],
            dst_ref=square_recv.at[grp * rows + row],
            send_sem=square_sems.at[0, mask, ahead, flip],
            recv_sem=square_sems.at[1, mask, ahead, flip],
            device_id=device(mask, lax.rem(plane + ahead, planes), lax.rem(core + flip, 2)),
            device_id_type=MESH,
        )

    def squares_to(ahead):
        for mask in range(groups):
            for flip in range(2):
                square_copy(mask, ahead, flip).start()

    def near_squares(action):
        for mask in range(groups):
            for flip in range(0 if mask else 1, 2):
                action(square_copy(mask, 0, flip))

    def finish_stats(slots, stats):
        parity = lane & 1
        column = lax.rem(grid_iota((pair, LANES), 0), wanted_dev)
        line = jnp.zeros((pair, LANES), jnp.float32)
        for kind in range(2):
            sums = jnp.sum(jnp.where(parity == kind, stats, 0.0), axis=1, keepdims=True)
            line = jnp.where(lane == column + kind * wanted_dev, sums, line)
        scales = jnp.sqrt(jnp.maximum(stats, LEAST))
        for index, slot in enumerate(slots):
            part = slice(index * wanted_dev, (index + 1) * wanted_dev)
            square_send[slot] = jnp.sum(line[part], axis=0, keepdims=True)
            if slot:
                stat_send[slot] = scales[part]

    nothing = jnp.zeros((pair, LANES), jnp.float32)
    early = plane < cdiv(planes, 2)

    shift_values = prepare((1, 2))

    def first(step, stats):
        for half in range(2):
            chunk = 2 * step + half
            for copy in loads(chunk):
                copy.wait()
            stats = compute((1, 2), shift_values, chunk, stats)
            if half == 0:
                for mask in (1, 2):
                    data_copy(mask, step).start()
        return stats

    stats = lax.fori_loop(0, chunks // 2, first, nothing)
    finish_stats((1, 2), stats)

    coef_wait(3)
    shift_other = prepare((3, 0))

    def second(step, stats):
        for half in range(2):
            stats = compute((3, 0), shift_other, 2 * step + half, stats)
            if half == 0:
                @pl.when(early)
                def _():
                    for mask in (1, 2):
                        data_copy(mask, chunks // 2 + step).start()
        return stats

    stats = lax.fori_loop(0, chunks // 2, second, nothing)
    finish_stats((3, 0), stats)

    for mask in (1, 2, 3):
        stat_copy(mask).start()
    near_squares(lambda copy: copy.start())

    if planes > 1:
        @pl.when(core == 0)
        def _():
            pl.semaphore_wait(barrier, planes - 1)

            def tell(ahead, carry):
                signal(plane_sem.at[plane], device(0, lax.rem(plane + ahead, planes), 0))
                return carry

            lax.fori_loop(1, planes, tell, 0)

    def far_squares(other, carry):
        @pl.when(core == 0)
        def _():
            pl.semaphore_wait(plane_sem.at[other], 1)
            signal(go_sem.at[other], device(0, plane, 1))

        @pl.when(lead)
        def _():
            pl.semaphore_wait(go_sem.at[other], 1)

        squares_to(lax.rem(other + planes - plane, planes))
        return carry

    lax.fori_loop(0, plane, far_squares, 0)

    @pl.when(jnp.logical_not(early))
    def _():
        def rest(chunk, carry):
            for mask in (1, 2):
                data_copy(mask, chunk).start()
            return carry

        lax.fori_loop(chunks // 2, chunks, rest, 0)

    def across(chunk, carry):
        data_copy(3, chunk).start()
        return carry

    lax.fori_loop(0, chunks, across, 0)
    lax.fori_loop(plane + 1, planes, far_squares, 0)

    for mask in (1, 2, 3):
        stat_copy(mask).wait()

    lane_dev = grid_iota((wanted_dev, LANES), 1)

    def take(masks, chunk, carry):
        for mask in masks:
            data_copy(mask, chunk).wait()
            for kind in range(2):
                scale = jnp.sum(
                    jnp.where(lane_dev == 2 * chunk + kind, stat_recv[mask], 0.0), axis=1, keepdims=True
                )
                codes = received[mask - 1, chunk, :, kind * inner_dev : (kind + 1) * inner_dev]
                size = decode(codes.astype(jnp.float32)).reshape(wanted_dev, TILE, inner_dev)
                put_out(kind, chunk, partner(mask), size * expand_rows(scale * (1.0 / PEAK), inner_dev))
        return carry

    lax.fori_loop(0, chunks, functools.partial(take, (1, 2)), 0)
    lax.fori_loop(0, chunks, functools.partial(take, (3,)), 0)

    near_squares(lambda copy: copy.wait())

    def far_wait(ahead, carry):
        for mask in range(groups):
            for flip in range(2):
                square_copy(mask, ahead, flip).wait()
        return carry

    lax.fori_loop(1, planes, far_wait, 0)
    square_recv[grp * rows + row] = square_send[0]
    total_ref[...] = jnp.sum(square_recv[...], axis=0)

    @pl.when(lead)
    def _():
        for copy in own_sends + relay_sends:
            copy.wait_send()


def finish_kernel(rows_total, ritz_in, resid_in, total_ref, ritz_out, resid_out, norm_ref, scaled, sems):
    wanted_dev, outer_dev, inner = ritz_in.shape
    pieces = sems.shape[1]
    several = outer_dev // pieces
    lanes = grid_iota((wanted_dev, LANES), 1)
    columns = grid_iota((wanted_dev, LANES), 0)
    total = jnp.broadcast_to(total_ref[...], (wanted_dev, LANES))
    unit = 1.0 / (SHIFT * SHIFT)

    def pick(lane):
        return jnp.sum(jnp.where(lanes == lane, total, 0.0), axis=1, keepdims=True) * unit

    ritz_squares = pick(columns) + 1.0
    resid_squares = pick(columns + wanted_dev)
    factor = jnp.sqrt(rows_total / ritz_squares)
    spot = expand_rows(factor * (1.0 / SHIFT), inner)
    copies = []
    for piece in range(pieces):
        span = slice(piece * several, (piece + 1) * several)
        for kind, (source, out) in enumerate(((ritz_in, ritz_out), (resid_in, resid_out))):
            scaled[kind, :, span] = source[:, span] * spot
            copy = pltpu.make_async_copy(scaled.at[kind, :, span], out.at[:, span], sems.at[kind, piece])
            copy.start()
            copies.append(copy)
    norms = jnp.broadcast_to(jnp.sqrt(resid_squares / ritz_squares), (wanted_dev, LANES))
    norm_ref[...] = jnp.sum(jnp.where(lanes == columns, norms, 0.0), axis=0)[:wanted_dev]
    for copy in copies:
        copy.wait()


def body(groups, rows, krylov_basis, krylov_image, tridiag_vectors, ritz_values):
    krylov_len, outer_dev, inner_dev = krylov_basis.shape
    wanted_dev = tridiag_vectors.shape[1]
    chunks = outer_dev // TILE
    block = wanted_dev * TILE
    planes = rows // 2
    assert groups == 4 and rows == 2 * planes and chunks % 2 == 0
    padded_len = cdiv(krylov_len, STEP) * STEP
    rows_total = float(outer_dev * inner_dev * groups * rows)
    f32, bf16 = jnp.float32, jnp.bfloat16
    dma, regular = pltpu.SemaphoreType.DMA, pltpu.SemaphoreType.REGULAR
    vmem = pl.BlockSpec(memory_space=pltpu.VMEM)
    hbm = pl.BlockSpec(memory_space=pltpu.HBM)
    parts = cdiv(padded_len, LANES)
    out = jax.ShapeDtypeStruct((wanted_dev, outer_dev, groups * inner_dev), f32)
    ritz, resid, total = pl.pallas_call(
        functools.partial(exchange_kernel, groups, rows),
        name="exchange",
        out_shape=(out, out, jax.ShapeDtypeStruct((1, LANES), f32)),
        in_specs=[hbm] * 4,
        out_specs=(vmem, vmem, vmem),
        scratch_shapes=[
            pltpu.VMEM((groups, wanted_dev, krylov_len), bf16),
            pltpu.VMEM((groups, 1, wanted_dev), bf16),
            pltpu.VMEM((2, chunks, padded_len, TILE, inner_dev), bf16),
            pltpu.VMEM((LANES, LANES * TILE), bf16),
            pltpu.VMEM((parts, 2 * wanted_dev, LANES * TILE), f32),
            pltpu.VMEM((2 * wanted_dev * TILE, padded_len * TILE), bf16),
            pltpu.VMEM((groups - 1, chunks, block, 2 * inner_dev), bf16),
            pltpu.VMEM((groups - 1, chunks, block, 2 * inner_dev), bf16),
            pltpu.VMEM((groups, wanted_dev, LANES), f32),
            pltpu.VMEM((groups, wanted_dev, LANES), f32),
            pltpu.VMEM((groups, 1, LANES), f32),
            pltpu.VMEM((groups * rows, 1, LANES), f32),
            dma((2,)),
            dma((6, 2)),
            dma((groups - 1, 2)),
            dma((2, chunks)),
            dma((2, groups - 1, chunks)),
            dma((2, groups)),
            dma((2, groups, planes, 2)),
            regular,
            regular((planes,)),
            regular((planes,)),
        ],
        compiler_params=pltpu.CompilerParams(
            collective_id=0, has_side_effects=True, vmem_limit_bytes=48 * MIB
        ),
    )(tridiag_vectors.T, ritz_values[None], krylov_basis, krylov_image)
    pieces = math.gcd(chunks, 8)
    return pl.pallas_call(
        functools.partial(finish_kernel, rows_total),
        name="finish",
        out_shape=(out, out, jax.ShapeDtypeStruct((wanted_dev,), f32)),
        in_specs=[vmem] * 3,
        out_specs=(hbm, hbm, vmem),
        scratch_shapes=[
            pltpu.VMEM((2, wanted_dev, outer_dev, groups * inner_dev), f32),
            dma((2, pieces)),
        ],
        compiler_params=pltpu.CompilerParams(vmem_limit_bytes=16 * MIB),
    )(ritz, resid, total)


def solution(mesh):
    placed = (P(None, "row", "grp"), P(None, "row", "grp"), P(None, "grp"), P("grp"))
    return jax.shard_map(
        functools.partial(body, mesh.shape["grp"], mesh.shape["row"]),
        mesh=mesh,
        in_specs=placed,
        out_specs=(P("grp", "row", None), P("grp", "row", None), P("grp")),
        check_vma=False,
    )
```

```python
import functools
import math

import jax
import jax.numpy as jnp
from jax import lax
from jax.experimental import pallas as pl
from jax.experimental.pallas import tpu as pltpu
from jax.sharding import PartitionSpec as P

MESH = pl.DeviceIdType.MESH
MIB = 1 << 20
TILE = 8
STEP = 16
LANES = 128
POWER = 13
PEAK = 2.0 ** (126.0 / POWER)
SHIFT = 2.0**30
LEAST = 1e-36


def cdiv(a, b):
    return (a + b - 1) // b


def grid_iota(shape, dim):
    return lax.broadcasted_iota(jnp.int32, shape, dim)


def expand_rows(cols, width):
    return jnp.broadcast_to(cols, (cols.shape[0], width)).reshape(cols.shape[0], 1, width)


def encode(cols, inverse):
    y = cols * inverse
    y2 = y * y
    y4 = y2 * y2
    y8 = y4 * y4
    return (y8 * y4) * y


def decode(codes):
    size = jnp.exp2(jnp.log(jnp.abs(codes)) * (1.0 / (POWER * math.log(2.0))))
    return jnp.where(codes < 0.0, -size, size)


def exchange_kernel(
    groups, rows,
    tridiag_ref, values_ref, basis_ref, image_ref,
    ritz_ref, resid_ref, total_ref,
    coefs, values, fields, spread, reps, expanded, coded, received,
    stat_send, stat_recv, square_send, square_recv,
    coef_load, coef_send, coef_recv, load_sem, send_sem, recv_sem, small_send, small_recv,
    ready_sem, order_sem,
):
    wanted_dev, krylov_len = tridiag_ref.shape
    chunks = fields.shape[0]
    pairs = chunks // 2
    padded_len = fields.shape[2]
    inner_dev = basis_ref.shape[2]
    steps = padded_len // STEP
    wide = STEP * TILE
    block = wanted_dev * TILE
    planes = rows // 2
    grp = lax.axis_index("grp")
    row = lax.axis_index("row")
    core = lax.rem(row, 2)
    plane = lax.div(row, 2)
    lead = core == 1

    def partner(mask):
        if mask == 0:
            return grp
        if mask == 1:
            return grp + 1 - 2 * lax.rem(grp, 2)
        if mask == 2:
            return lax.rem(grp + 2, groups)
        return groups - 1 - grp

    def device(mask, at_plane, at_core):
        return {"grp": partner(mask), "row": 2 * at_plane + at_core}

    def signal(sem, where):
        pl.semaphore_signal(sem, inc=1, device_id=where, device_id_type=MESH)

    barrier = pltpu.get_barrier_semaphore()
    for mask in (1, 2):
        signal(barrier, device(mask, plane, 1))

    coef_loads = [
        pltpu.make_async_copy(tridiag_ref, coefs.at[0], coef_load.at[0]),
        pltpu.make_async_copy(values_ref, values.at[0], coef_load.at[1]),
    ]
    for copy in coef_loads:
        copy.start()

    @pl.when(core == 0)
    def _():
        signal(barrier, device(0, plane, 1))

        def greet(ahead, carry):
            signal(barrier, device(0, lax.rem(plane + ahead, planes), 0))
            return carry

        lax.fori_loop(1, planes, greet, 0)

    for chunk in range(chunks):
        for which, ref in enumerate((basis_ref, image_ref)):
            pltpu.make_async_copy(
                ref.at[:, chunk * TILE : (chunk + 1) * TILE, :],
                fields.at[chunk, which, pl.ds(0, krylov_len)],
                load_sem.at[chunk // 2],
            ).start()

    def land(ref, sem):
        pltpu.make_async_copy(ref, ref, sem).wait()

    def load_wait(step):
        land(fields.at[pl.ds(2 * step, 2), :, pl.ds(0, krylov_len)], load_sem.at[step])

    if padded_len > krylov_len:
        for chunk in range(chunks):
            for which in range(2):
                fields[chunk, which, pl.ds(krylov_len, padded_len - krylov_len)] = jnp.zeros(
                    (padded_len - krylov_len, TILE, inner_dev), jnp.bfloat16
                )
    shape = spread.shape
    spread[...] = jnp.where(
        lax.shift_right_logical(grid_iota(shape, 1), 3) == grid_iota(shape, 0), SHIFT, 0.0
    ).astype(jnp.bfloat16)

    for copy in coef_loads:
        copy.wait()

    def coef_copies(source, slot, mask, at_core):
        return [
            pltpu.make_async_remote_copy(
                src_ref=ref.at[source],
                dst_ref=ref.at[slot],
                send_sem=coef_send.at[kind],
                recv_sem=coef_recv.at[slot - 1, kind],
                device_id=device(mask, plane, at_core),
                device_id_type=MESH,
            )
            for kind, ref in enumerate((coefs, values))
        ]

    own_sends = [
        copy
        for mask in (1, 2)
        for at_core in (1, 0)
        for copy in coef_copies(0, mask, mask, at_core)
    ]
    relay_sends = [copy for at_core in (1, 0) for copy in coef_copies(1, 3, 2, at_core)]

    def coef_wait(slot):
        for copy in coef_copies(0, slot, 1, 1):
            copy.wait_recv()

    @pl.when(lead)
    def _():
        pl.semaphore_wait(barrier, 5)
        for copy in own_sends:
            copy.start()
        signal(ready_sem, device(0, plane, 0))
        coef_wait(1)
        for copy in relay_sends:
            copy.start()
        coef_wait(2)

    @pl.when(core == 0)
    def _():
        pl.semaphore_wait(ready_sem, 1)
        coef_wait(1)
        coef_wait(2)

    near = grid_iota((wanted_dev, wanted_dev), 0) == grid_iota((wanted_dev, wanted_dev), 1)
    same = (grid_iota((TILE, wide), 1) & (TILE - 1)) == grid_iota((TILE, wide), 0)
    per_part = LANES // STEP
    pair = 2 * wanted_dev
    lane = grid_iota((pair, LANES), 1)

    def prepare(slots):
        shifts = []
        for slot in slots:
            spot = jnp.broadcast_to(values[slot].astype(jnp.float32), (wanted_dev, wanted_dev))
            shifts.append(jnp.sum(jnp.where(near, spot, 0.0), axis=1, keepdims=True))
        shift_values = expand_rows(jnp.concatenate(shifts, axis=0), inner_dev)
        both = jnp.concatenate([coefs[slot] for slot in slots], axis=0)
        for part in range(cdiv(krylov_len, LANES)):
            piece = both[:, part * LANES : min((part + 1) * LANES, krylov_len)]
            reps[part] = jnp.dot(piece, spread[: piece.shape[1]], preferred_element_type=jnp.float32)
        for step in range(steps):
            at = (step % per_part) * wide
            spot = reps[step // per_part, :, at : at + wide]
            spot = jnp.where(same[None], spot.reshape(pair, 1, wide), 0.0)
            expanded[:, step * wide : (step + 1) * wide] = spot.reshape(pair * TILE, wide).astype(jnp.bfloat16)
        return shift_values

    def compute(slots, shift_values, step, stats):
        both = jnp.concatenate(
            [
                fields[2 * step + half, which].reshape(padded_len * TILE, inner_dev)
                for half in range(2)
                for which in range(2)
            ],
            axis=1,
        )
        product = jnp.dot(expanded[...], both, preferred_element_type=jnp.float32)
        product = product.reshape(pair, TILE, 4 * inner_dev)
        for half in range(2):
            chunk = 2 * step + half
            at = 2 * half * inner_dev
            ritz = product[:, :, at : at + inner_dev]
            resid = product[:, :, at + inner_dev : at + 2 * inner_dev] - shift_values * ritz
            for kind, cols in enumerate((ritz, resid)):
                squares = jnp.sum(jnp.sum(cols * cols, axis=1), axis=1, keepdims=True)
                stats = jnp.where(lane == 2 * chunk + kind, squares, stats)
                inverse = expand_rows(PEAK / jnp.sqrt(jnp.maximum(squares, LEAST)), inner_dev)
                for index, slot in enumerate(slots):
                    part = slice(index * wanted_dev, (index + 1) * wanted_dev)
                    if slot == 0:
                        put_out(kind, chunk, grp, cols[part])
                    else:
                        coded[slot - 1, chunk, :, kind * inner_dev : (kind + 1) * inner_dev] = encode(
                            cols[part], inverse[part]
                        ).reshape(block, inner_dev).astype(jnp.bfloat16)
        return stats

    def put_out(kind, chunk, source, cols):
        span = pl.ds(pl.multiple_of(chunk * TILE, TILE), TILE)
        lanes = pl.ds(pl.multiple_of(source * inner_dev, inner_dev), inner_dev)
        (ritz_ref, resid_ref)[kind][:, span, lanes] = cols

    def data_copy(mask, step):
        span = pl.ds(2 * step, 2)
        return pltpu.make_async_remote_copy(
            src_ref=coded.at[mask - 1, span],
            dst_ref=received.at[mask - 1, span],
            send_sem=send_sem,
            recv_sem=recv_sem.at[0 if mask < 3 else 1, step],
            device_id=device(mask, plane, core),
            device_id_type=MESH,
        )

    def stat_copy(mask):
        return pltpu.make_async_remote_copy(
            src_ref=stat_send.at[mask],
            dst_ref=stat_recv.at[mask],
            send_sem=small_send.at[0],
            recv_sem=small_recv.at[0],
            device_id=device(mask, plane, core),
            device_id_type=MESH,
        )

    def squares_to(mask, at_plane, flip):
        pltpu.make_async_remote_copy(
            src_ref=square_send.at[mask],
            dst_ref=square_recv.at[grp * rows + row],
            send_sem=small_send.at[1],
            recv_sem=small_recv.at[1],
            device_id=device(mask, at_plane, lax.rem(core + flip, 2)),
            device_id_type=MESH,
        ).start()

    def far_squares(at_plane, carry):
        for mask in range(groups):
            for flip in range(2):
                squares_to(mask, at_plane, flip)
        return carry

    def agree(side, count):
        @pl.when(core == 0)
        def _():
            pl.semaphore_wait(order_sem.at[side], count)
            signal(order_sem.at[side], device(0, plane, 1))

        @pl.when(lead)
        def _():
            pl.semaphore_wait(order_sem.at[side], 1)

    def finish_stats(slots, stats):
        parity = lane & 1
        column = lax.rem(grid_iota((pair, LANES), 0), wanted_dev)
        line = jnp.zeros((pair, LANES), jnp.float32)
        for kind in range(2):
            sums = jnp.sum(jnp.where(parity == kind, stats, 0.0), axis=1, keepdims=True)
            line = jnp.where(lane == column + kind * wanted_dev, sums, line)
        scales = jnp.sqrt(jnp.maximum(stats, LEAST))
        for index, slot in enumerate(slots):
            part = slice(index * wanted_dev, (index + 1) * wanted_dev)
            square_send[slot] = jnp.sum(line[part], axis=0, keepdims=True)
            if slot:
                stat_send[slot] = scales[part]

    nothing = jnp.zeros((pair, LANES), jnp.float32)
    early = plane == 0

    shift_values = prepare((1, 2))

    def first(step, stats):
        load_wait(step)
        stats = compute((1, 2), shift_values, step, stats)
        for mask in (1, 2):
            data_copy(mask, step).start()
        return stats

    stats = lax.fori_loop(0, pairs, first, nothing)
    finish_stats((1, 2), stats)

    coef_wait(3)
    if planes > 1:
        @pl.when(core == 0)
        def _():
            pl.semaphore_wait(barrier, planes - 1)

            def lower(other, carry):
                signal(order_sem.at[1], device(0, other, 0))
                return carry

            def upper(other, carry):
                signal(order_sem.at[0], device(0, other, 0))
                return carry

            lax.fori_loop(plane + 1, planes, upper, 0)
            lax.fori_loop(0, plane, lower, 0)

    shift_other = prepare((3, 0))

    def second(step, stats):
        stats = compute((3, 0), shift_other, step, stats)

        @pl.when(jnp.logical_and(early, lax.rem(step, 2) == 1))
        def _():
            data_copy(3, lax.div(step, 2)).start()

        return stats

    stats = lax.fori_loop(0, pairs, second, nothing)
    finish_stats((3, 0), stats)

    for mask in (1, 2, 3):
        stat_copy(mask).start()
    for mask in range(groups):
        for flip in range(0 if mask else 1, 2):
            squares_to(mask, plane, flip)
    if planes > 1:
        @pl.when(plane > 0)
        def _():
            agree(0, plane)
            lax.fori_loop(0, plane, far_squares, 0)

    def across(step, carry):
        data_copy(3, step).start()
        return carry

    lax.fori_loop(jnp.where(early, pairs // 2, 0), pairs, across, 0)

    land(stat_recv.at[pl.ds(1, groups - 1)], small_recv.at[0])

    lane_dev = grid_iota((wanted_dev, LANES), 1)

    def take(masks, step, carry):
        land(
            received.at[pl.ds(masks[0] - 1, len(masks)), pl.ds(2 * step, 2)],
            recv_sem.at[0 if masks[0] < 3 else 1, step],
        )
        for half in range(2):
            chunk = 2 * step + half
            for mask in masks:
                for kind in range(2):
                    scale = jnp.sum(
                        jnp.where(lane_dev == 2 * chunk + kind, stat_recv[mask], 0.0), axis=1, keepdims=True
                    )
                    codes = received[mask - 1, chunk, :, kind * inner_dev : (kind + 1) * inner_dev]
                    size = decode(codes.astype(jnp.float32)).reshape(wanted_dev, TILE, inner_dev)
                    put_out(kind, chunk, partner(mask), size * expand_rows(scale * (1.0 / PEAK), inner_dev))
        return carry

    lax.fori_loop(0, pairs, functools.partial(take, (1, 2)), 0)
    if planes > 1:
        @pl.when(plane < planes - 1)
        def _():
            agree(1, planes - 1 - plane)
            lax.fori_loop(plane + 1, planes, far_squares, 0)

    lax.fori_loop(0, pairs, functools.partial(take, (3,)), 0)

    others = groups * rows - 1
    land(square_recv.at[pl.ds(0, others)], small_recv.at[1])
    land(square_recv.at[pl.ds(0, others)], small_send.at[1])
    land(stat_send.at[pl.ds(1, groups - 1)], small_send.at[0])
    land(coded, send_sem)
    square_recv[grp * rows + row] = square_send[0]
    total_ref[...] = jnp.sum(square_recv[...], axis=0)

    @pl.when(lead)
    def _():
        for kind, ref in enumerate((coefs, values)):
            land(ref, coef_send.at[kind])


def finish_kernel(rows_total, ritz_in, resid_in, total_ref, ritz_out, resid_out, norm_ref, scaled, sems):
    wanted_dev, outer_dev, inner = ritz_in.shape
    pieces = math.gcd(outer_dev // TILE, 8)
    several = outer_dev // pieces
    lanes = grid_iota((wanted_dev, LANES), 1)
    columns = grid_iota((wanted_dev, LANES), 0)
    total = jnp.broadcast_to(total_ref[...], (wanted_dev, LANES))
    unit = 1.0 / (SHIFT * SHIFT)

    def pick(lane):
        return jnp.sum(jnp.where(lanes == lane, total, 0.0), axis=1, keepdims=True) * unit

    ritz_squares = pick(columns) + 1.0
    resid_squares = pick(columns + wanted_dev)
    factor = jnp.sqrt(rows_total / ritz_squares)
    spot = expand_rows(factor * (1.0 / SHIFT), inner)
    for piece in range(pieces):
        span = slice(piece * several, (piece + 1) * several)
        for kind, (source, out) in enumerate(((ritz_in, ritz_out), (resid_in, resid_out))):
            scaled[kind, :, span] = source[:, span] * spot
            copy = pltpu.make_async_copy(scaled.at[kind, :, span], out.at[:, span], sems.at[kind])
            copy.start()
    norms = jnp.broadcast_to(jnp.sqrt(resid_squares / ritz_squares), (wanted_dev, LANES))
    norm_ref[...] = jnp.sum(jnp.where(lanes == columns, norms, 0.0), axis=0)[:wanted_dev]
    for kind, out in enumerate((ritz_out, resid_out)):
        pltpu.make_async_copy(scaled.at[kind], out, sems.at[kind]).wait()


def body(groups, rows, krylov_basis, krylov_image, tridiag_vectors, ritz_values):
    krylov_len, outer_dev, inner_dev = krylov_basis.shape
    wanted_dev = tridiag_vectors.shape[1]
    chunks = outer_dev // TILE
    block = wanted_dev * TILE
    planes = rows // 2
    assert groups == 4 and rows == 2 * planes and chunks % 2 == 0
    padded_len = cdiv(krylov_len, STEP) * STEP
    rows_total = float(outer_dev * inner_dev * groups * rows)
    f32, bf16 = jnp.float32, jnp.bfloat16
    dma, regular = pltpu.SemaphoreType.DMA, pltpu.SemaphoreType.REGULAR
    vmem = pl.BlockSpec(memory_space=pltpu.VMEM)
    hbm = pl.BlockSpec(memory_space=pltpu.HBM)
    parts = cdiv(padded_len, LANES)
    out = jax.ShapeDtypeStruct((wanted_dev, outer_dev, groups * inner_dev), f32)
    ritz, resid, total = pl.pallas_call(
        functools.partial(exchange_kernel, groups, rows),
        name="exchange",
        out_shape=(out, out, jax.ShapeDtypeStruct((1, LANES), f32)),
        in_specs=[hbm] * 4,
        out_specs=(vmem, vmem, vmem),
        scratch_shapes=[
            pltpu.VMEM((6, wanted_dev, krylov_len), bf16),
            pltpu.VMEM((6, 1, wanted_dev), bf16),
            pltpu.VMEM((chunks, 2, padded_len, TILE, inner_dev), bf16),
            pltpu.VMEM((LANES, LANES * TILE), bf16),
            pltpu.VMEM((parts, 2 * wanted_dev, LANES * TILE), f32),
            pltpu.VMEM((2 * wanted_dev * TILE, padded_len * TILE), bf16),
            pltpu.VMEM((groups - 1, chunks, block, 2 * inner_dev), bf16),
            pltpu.VMEM((groups - 1, chunks, block, 2 * inner_dev), bf16),
            pltpu.VMEM((groups, wanted_dev, LANES), f32),
            pltpu.VMEM((groups, wanted_dev, LANES), f32),
            pltpu.VMEM((groups, 1, LANES), f32),
            pltpu.VMEM((groups * rows, 1, LANES), f32),
            dma((2,)),
            dma((2,)),
            dma((groups - 1, 2)),
            dma((chunks // 2,)),
            dma,
            dma((2, chunks // 2)),
            dma((2,)),
            dma((2,)),
            regular,
            regular((2,)),
        ],
        compiler_params=pltpu.CompilerParams(
            collective_id=0, has_side_effects=True, vmem_limit_bytes=48 * MIB
        ),
    )(*[pltpu.with_memory_space_constraint(x, pltpu.HBM) for x in (tridiag_vectors.T, ritz_values[None])], krylov_basis, krylov_image)
    return pl.pallas_call(
        functools.partial(finish_kernel, rows_total),
        name="finish",
        out_shape=(out, out, jax.ShapeDtypeStruct((wanted_dev,), f32)),
        in_specs=[vmem] * 3,
        out_specs=(hbm, hbm, vmem),
        scratch_shapes=[
            pltpu.VMEM((2, wanted_dev, outer_dev, groups * inner_dev), f32),
            dma((2,)),
        ],
        compiler_params=pltpu.CompilerParams(vmem_limit_bytes=16 * MIB),
    )(ritz, resid, total)


def solution(mesh):
    placed = (P(None, "row", "grp"), P(None, "row", "grp"), P(None, "grp"), P("grp"))
    return jax.shard_map(
        functools.partial(body, mesh.shape["grp"], mesh.shape["row"]),
        mesh=mesh,
        in_specs=placed,
        out_specs=(P("grp", "row", None), P("grp", "row", None), P("grp")),
        check_vma=False,
    )
```

```python
import functools
import math

import jax
import jax.numpy as jnp
from jax import lax
from jax.experimental import pallas as pl
from jax.experimental.pallas import tpu as pltpu
from jax.sharding import PartitionSpec as P

MESH = pl.DeviceIdType.MESH
MIB = 1 << 20
TILE = 8
STEP = 16
LANES = 128
POWER = 13
PEAK = 2.0 ** (126.0 / POWER)
SHIFT = 2.0**30
LEAST = 1e-36


def cdiv(a, b):
    return (a + b - 1) // b


def grid_iota(shape, dim):
    return lax.broadcasted_iota(jnp.int32, shape, dim)


def expand_rows(cols, width):
    return jnp.broadcast_to(cols, (cols.shape[0], width)).reshape(cols.shape[0], 1, width)


def encode(cols, inverse):
    y = cols * inverse
    y2 = y * y
    y4 = y2 * y2
    y8 = y4 * y4
    return (y8 * y4) * y


def decode(codes):
    size = jnp.exp2(jnp.log(jnp.abs(codes)) * (1.0 / (POWER * math.log(2.0))))
    return jnp.where(codes < 0.0, -size, size)


def exchange_kernel(
    groups, rows, rows_total,
    tridiag_ref, values_ref, basis_ref, image_ref,
    ritz_ref, resid_ref, factor_ref, norm_ref,
    coefs, values, fields, spread, expanded, coded, received,
    stat_send, stat_recv, square_send, square_recv,
    coef_load, coef_send, coef_recv, load_sem, send_sem, recv_sem, small_send, small_recv,
    ready_sem, order_sem,
):
    wanted_dev, krylov_len = tridiag_ref.shape
    chunks = fields.shape[0]
    pairs = chunks // 2
    padded_len = fields.shape[2]
    inner_dev = basis_ref.shape[2]
    steps = padded_len // STEP
    wide = STEP * TILE
    block = wanted_dev * TILE
    planes = rows // 2
    grp = lax.axis_index("grp")
    row = lax.axis_index("row")
    core = lax.rem(row, 2)
    plane = lax.div(row, 2)
    lead = core == 1

    def partner(mask):
        if mask == 0:
            return grp
        if mask == 1:
            return grp + 1 - 2 * lax.rem(grp, 2)
        if mask == 2:
            return lax.rem(grp + 2, groups)
        return groups - 1 - grp

    def device(mask, at_plane, at_core):
        return {"grp": partner(mask), "row": 2 * at_plane + at_core}

    def signal(sem, where):
        pl.semaphore_signal(sem, inc=1, device_id=where, device_id_type=MESH)

    barrier = pltpu.get_barrier_semaphore()
    for mask in (1, 2):
        signal(barrier, device(mask, plane, 1))

    coef_loads = [
        pltpu.make_async_copy(tridiag_ref, coefs.at[0], coef_load.at[0]),
        pltpu.make_async_copy(values_ref, values.at[0], coef_load.at[1]),
    ]
    for copy in coef_loads:
        copy.start()

    @pl.when(core == 0)
    def _():
        signal(barrier, device(0, plane, 1))

        def greet(ahead, carry):
            signal(barrier, device(0, lax.rem(plane + ahead, planes), 0))
            return carry

        lax.fori_loop(1, planes, greet, 0)

    for chunk in range(chunks):
        for which, ref in enumerate((basis_ref, image_ref)):
            pltpu.make_async_copy(
                ref.at[:, chunk * TILE : (chunk + 1) * TILE, :],
                fields.at[chunk, which, pl.ds(0, krylov_len)],
                load_sem.at[chunk // 2],
            ).start()

    def land(ref, sem):
        pltpu.make_async_copy(ref, ref, sem).wait()

    def load_wait(step):
        land(fields.at[pl.ds(2 * step, 2), :, pl.ds(0, krylov_len)], load_sem.at[step])

    if padded_len > krylov_len:
        for chunk in range(chunks):
            for which in range(2):
                fields[chunk, which, pl.ds(krylov_len, padded_len - krylov_len)] = jnp.zeros(
                    (padded_len - krylov_len, TILE, inner_dev), jnp.bfloat16
                )
    shape = spread.shape
    spread[...] = jnp.where(
        lax.shift_right_logical(grid_iota(shape, 1), 3) == grid_iota(shape, 0), SHIFT, 0.0
    ).astype(jnp.bfloat16)

    for copy in coef_loads:
        copy.wait()

    def coef_copies(source, slot, mask, at_core):
        return [
            pltpu.make_async_remote_copy(
                src_ref=ref.at[source],
                dst_ref=ref.at[slot],
                send_sem=coef_send.at[kind],
                recv_sem=coef_recv.at[slot - 1, kind],
                device_id=device(mask, plane, at_core),
                device_id_type=MESH,
            )
            for kind, ref in enumerate((coefs, values))
        ]

    own_sends = [
        copy
        for mask in (1, 2)
        for at_core in (1, 0)
        for copy in coef_copies(0, mask, mask, at_core)
    ]
    relay_sends = [copy for at_core in (1, 0) for copy in coef_copies(1, 3, 2, at_core)]

    def coef_wait(slot):
        for copy in coef_copies(0, slot, 1, 1):
            copy.wait_recv()

    @pl.when(lead)
    def _():
        pl.semaphore_wait(barrier, 5)
        for copy in own_sends:
            copy.start()
        signal(ready_sem, device(0, plane, 0))
        coef_wait(1)
        for copy in relay_sends:
            copy.start()
        coef_wait(2)

    @pl.when(core == 0)
    def _():
        pl.semaphore_wait(ready_sem, 1)
        coef_wait(1)
        coef_wait(2)

    near = grid_iota((wanted_dev, wanted_dev), 0) == grid_iota((wanted_dev, wanted_dev), 1)
    same = (grid_iota((TILE, wide), 1) & (TILE - 1)) == grid_iota((TILE, wide), 0)
    per_part = LANES // STEP
    pair = 2 * wanted_dev
    lane = grid_iota((pair, LANES), 1)

    def prepare(slots):
        shifts = []
        for slot in slots:
            spot = jnp.broadcast_to(values[slot].astype(jnp.float32), (wanted_dev, wanted_dev))
            shifts.append(jnp.sum(jnp.where(near, spot, 0.0), axis=1, keepdims=True))
        shift_values = expand_rows(jnp.concatenate(shifts, axis=0), inner_dev)
        both = jnp.concatenate([coefs[slot] for slot in slots], axis=0)
        for part in range(cdiv(krylov_len, LANES)):
            piece = both[:, part * LANES : min((part + 1) * LANES, krylov_len)]
            wider = jnp.dot(piece, spread[: piece.shape[1]], preferred_element_type=jnp.float32)
            for step in range(part * per_part, min((part + 1) * per_part, steps)):
                at = (step % per_part) * wide
                spot = jnp.where(same[None], wider[:, at : at + wide].reshape(pair, 1, wide), 0.0)
                expanded[:, step * wide : (step + 1) * wide] = spot.reshape(pair * TILE, wide).astype(jnp.bfloat16)
        return shift_values

    def compute(slots, shift_values, start, count, stats):
        both = jnp.concatenate(
            [
                fields[start + more, which].reshape(padded_len * TILE, inner_dev)
                for more in range(count)
                for which in range(2)
            ],
            axis=1,
        )
        product = jnp.dot(expanded[...], both, preferred_element_type=jnp.float32)
        product = product.reshape(pair, TILE, 2 * count * inner_dev)
        for more in range(count):
            chunk = start + more
            at = 2 * more * inner_dev
            ritz = product[:, :, at : at + inner_dev]
            resid = product[:, :, at + inner_dev : at + 2 * inner_dev] - shift_values * ritz
            for kind, cols in enumerate((ritz, resid)):
                squares = jnp.sum(jnp.sum(cols * cols, axis=1), axis=1, keepdims=True)
                stats = jnp.where(lane == 2 * chunk + kind, squares, stats)
                inverse = expand_rows(PEAK / jnp.sqrt(jnp.maximum(squares, LEAST)), inner_dev)
                for index, slot in enumerate(slots):
                    part = slice(index * wanted_dev, (index + 1) * wanted_dev)
                    if slot == 0:
                        put_out(kind, chunk, grp, cols[part])
                    else:
                        coded[slot - 1, chunk, :, kind * inner_dev : (kind + 1) * inner_dev] = encode(
                            cols[part], inverse[part]
                        ).reshape(block, inner_dev).astype(jnp.bfloat16)
        return stats

    def put_out(kind, chunk, source, cols):
        span = pl.ds(pl.multiple_of(chunk * TILE, TILE), TILE)
        lanes = pl.ds(pl.multiple_of(source * inner_dev, inner_dev), inner_dev)
        (ritz_ref, resid_ref)[kind][:, span, lanes] = cols

    def data_copy(mask, start, count=2):
        span = pl.ds(start, count)
        return pltpu.make_async_remote_copy(
            src_ref=coded.at[mask - 1, span],
            dst_ref=received.at[mask - 1, span],
            send_sem=send_sem,
            recv_sem=recv_sem.at[mask - 1, lax.div(start, 2)],
            device_id=device(mask, plane, core),
            device_id_type=MESH,
        )

    def stat_copy(mask):
        return pltpu.make_async_remote_copy(
            src_ref=stat_send.at[mask],
            dst_ref=stat_recv.at[mask],
            send_sem=small_send.at[0],
            recv_sem=small_recv.at[0 if mask < 3 else 2],
            device_id=device(mask, plane, core),
            device_id_type=MESH,
        )

    def squares_to(mask, at_plane, flip):
        pltpu.make_async_remote_copy(
            src_ref=square_send.at[mask],
            dst_ref=square_recv.at[grp * rows + row],
            send_sem=small_send.at[1],
            recv_sem=small_recv.at[1],
            device_id=device(mask, at_plane, lax.rem(core + flip, 2)),
            device_id_type=MESH,
        ).start()

    def far_squares(at_plane, carry):
        for mask in range(groups):
            for flip in range(2):
                squares_to(mask, at_plane, flip)
        return carry

    def agree(side, count):
        @pl.when(core == 0)
        def _():
            pl.semaphore_wait(order_sem.at[side], count)
            signal(order_sem.at[side], device(0, plane, 1))

        @pl.when(lead)
        def _():
            pl.semaphore_wait(order_sem.at[side], 1)

    def finish_stats(slots, stats):
        parity = lane & 1
        column = lax.rem(grid_iota((pair, LANES), 0), wanted_dev)
        line = jnp.zeros((pair, LANES), jnp.float32)
        for kind in range(2):
            sums = jnp.sum(jnp.where(parity == kind, stats, 0.0), axis=1, keepdims=True)
            line = jnp.where(lane == column + kind * wanted_dev, sums, line)
        scales = jnp.sqrt(jnp.maximum(stats, LEAST))
        for index, slot in enumerate(slots):
            part = slice(index * wanted_dev, (index + 1) * wanted_dev)
            square_send[slot] = jnp.sum(line[part], axis=0, keepdims=True)
            if slot:
                stat_send[slot] = scales[part]

    nothing = jnp.zeros((pair, LANES), jnp.float32)
    shift_values = prepare((1, 2))
    def first(step, stats):
        load_wait(step)
        stats = compute((1, 2), shift_values, 2 * step, 2, stats)
        @pl.when(step < pairs - 1)
        def _():
            for mask in (1, 2):
                data_copy(mask, 2 * step).start()

        return stats

    stats = lax.fori_loop(0, pairs, first, nothing)
    finish_stats((1, 2), stats)
    for mask in (1, 2):
        stat_copy(mask).start()
    data_copy(2, chunks - 2).start()

    coef_wait(3)
    if planes > 1:
        @pl.when(core == 0)
        def _():
            pl.semaphore_wait(barrier, planes - 1)

            def lower(other, carry):
                signal(order_sem.at[1], device(0, other, 0))
                return carry

            def upper(other, carry):
                signal(order_sem.at[0], device(0, other, 0))
                return carry

            lax.fori_loop(plane + 1, planes, upper, 0)
            lax.fori_loop(0, plane, lower, 0)

    shift_other = prepare((3, 0))

    def second(step, stats):
        stats = compute((3, 0), shift_other, 2 * step, 2, stats)

        @pl.when(lax.rem(step, 2) == 0)
        def _():
            data_copy(3, step).start()

        return stats

    stats = lax.fori_loop(0, pairs, second, nothing)
    finish_stats((3, 0), stats)

    stat_copy(3).start()
    for mask in range(groups):
        for flip in range(0 if mask else 1, 2):
            squares_to(mask, plane, flip)
    if planes > 1:
        @pl.when(plane > 0)
        def _():
            agree(0, plane)
            lax.fori_loop(0, plane, far_squares, 0)

    def across(step, carry):
        data_copy(3, 2 * step).start()
        return carry

    lax.fori_loop(cdiv(pairs, 2), pairs, across, 0)
    data_copy(1, chunks - 2).start()

    if planes > 1:
        @pl.when(plane < planes - 1)
        def _():
            agree(1, planes - 1 - plane)
            lax.fori_loop(plane + 1, planes, far_squares, 0)

    land(stat_recv.at[pl.ds(1, 2)], small_recv.at[0])

    lane_dev = grid_iota((wanted_dev, LANES), 1)

    def take(masks, step, carry):
        for mask in masks:
            land(received.at[mask - 1, pl.ds(2 * step, 2)], recv_sem.at[mask - 1, step])
        for half in range(2):
            chunk = 2 * step + half
            for mask in masks:
                for kind in range(2):
                    scale = jnp.sum(
                        jnp.where(lane_dev == 2 * chunk + kind, stat_recv[mask], 0.0), axis=1, keepdims=True
                    )
                    codes = received[mask - 1, chunk, :, kind * inner_dev : (kind + 1) * inner_dev]
                    size = decode(codes.astype(jnp.float32)).reshape(wanted_dev, TILE, inner_dev)
                    put_out(kind, chunk, partner(mask), size * expand_rows(scale * (1.0 / PEAK), inner_dev))
        return carry

    lax.fori_loop(0, pairs - 1, functools.partial(take, (1, 2)), 0)
    take((2,), pairs - 1, 0)
    land(stat_recv.at[3], small_recv.at[2])
    lax.fori_loop(0, pairs, functools.partial(take, (3,)), 0)

    others = groups * rows - 1
    land(square_recv.at[pl.ds(0, others)], small_recv.at[1])
    square_recv[grp * rows + row] = square_send[0]
    total = jnp.broadcast_to(jnp.sum(square_recv[...], axis=0), (wanted_dev, LANES))
    column = grid_iota((wanted_dev, LANES), 0)
    unit = 1.0 / (SHIFT * SHIFT)
    ritz_squares, resid_squares = (
        jnp.sum(jnp.where(lane_dev == column + kind * wanted_dev, total, 0.0), axis=1, keepdims=True) * unit
        for kind in range(2)
    )
    ritz_squares = ritz_squares + 1.0
    factor_ref[...] = jnp.broadcast_to(
        jnp.sqrt(rows_total / ritz_squares) * (1.0 / SHIFT), (wanted_dev, LANES)
    )
    norms = jnp.broadcast_to(jnp.sqrt(resid_squares / ritz_squares), (wanted_dev, LANES))
    norm_ref[...] = jnp.sum(jnp.where(lane_dev == column, norms, 0.0), axis=0, keepdims=True)

    land(square_recv.at[pl.ds(0, others)], small_send.at[1])
    land(stat_send.at[pl.ds(1, groups - 1)], small_send.at[0])

    @pl.when(lead)
    def _():
        for kind, ref in enumerate((coefs, values)):
            land(ref, coef_send.at[kind])

    take((1,), pairs - 1, 0)
    land(coded, send_sem)


def finish_kernel(ritz_in, resid_in, factor_ref, norm_in, ritz_out, resid_out, norm_out, scaled, norm, sems):
    wanted_dev, _, inner = ritz_in.shape
    norm[...] = norm_in[0, :wanted_dev]
    norm_copy = pltpu.make_async_copy(norm, norm_out, sems.at[2])
    norm_copy.start()
    for column in range(wanted_dev):
        span = slice(column, column + 1)
        spot = jnp.broadcast_to(factor_ref[span], (TILE, LANES))
        spot = jnp.concatenate([spot] * (inner // LANES), axis=1)[None]
        for kind, (source, out) in enumerate(((ritz_in, ritz_out), (resid_in, resid_out))):
            for at in range(0, source.shape[1], TILE):
                scaled[kind, span, at : at + TILE] = source[span, at : at + TILE] * spot
            pltpu.make_async_copy(scaled.at[kind, span], out.at[span], sems.at[kind]).start()
    norm_copy.wait()
    for kind, out in enumerate((ritz_out, resid_out)):
        pltpu.make_async_copy(scaled.at[kind], out, sems.at[kind]).wait()


def body(groups, rows, krylov_basis, krylov_image, tridiag_vectors, ritz_values):
    krylov_len, outer_dev, inner_dev = krylov_basis.shape
    wanted_dev = tridiag_vectors.shape[1]
    chunks = outer_dev // TILE
    block = wanted_dev * TILE
    planes = rows // 2
    assert groups == 4 and rows == 2 * planes and chunks % 2 == 0
    padded_len = cdiv(krylov_len, STEP) * STEP
    rows_total = float(outer_dev * inner_dev * groups * rows)
    f32, bf16 = jnp.float32, jnp.bfloat16
    dma, regular = pltpu.SemaphoreType.DMA, pltpu.SemaphoreType.REGULAR
    vmem = pl.BlockSpec(memory_space=pltpu.VMEM)
    hbm = pl.BlockSpec(memory_space=pltpu.HBM)
    out = jax.ShapeDtypeStruct((wanted_dev, outer_dev, groups * inner_dev), f32)
    ritz, resid, factor, norms = pl.pallas_call(
        functools.partial(exchange_kernel, groups, rows, rows_total),
        name="exchange",
        out_shape=(
            out, out, jax.ShapeDtypeStruct((wanted_dev, LANES), f32), jax.ShapeDtypeStruct((1, LANES), f32),
        ),
        in_specs=[hbm] * 4,
        out_specs=(vmem,) * 4,
        scratch_shapes=[
            pltpu.VMEM((6, wanted_dev, krylov_len), bf16),
            pltpu.VMEM((6, 1, wanted_dev), bf16),
            pltpu.VMEM((chunks, 2, padded_len, TILE, inner_dev), bf16),
            pltpu.VMEM((LANES, LANES * TILE), bf16),
            pltpu.VMEM((2 * wanted_dev * TILE, padded_len * TILE), bf16),
            pltpu.VMEM((groups - 1, chunks, block, 2 * inner_dev), bf16),
            pltpu.VMEM((groups - 1, chunks, block, 2 * inner_dev), bf16),
            pltpu.VMEM((groups, wanted_dev, LANES), f32),
            pltpu.VMEM((groups, wanted_dev, LANES), f32),
            pltpu.VMEM((groups, 1, LANES), f32),
            pltpu.VMEM((groups * rows, 1, LANES), f32),
            dma((2,)),
            dma((2,)),
            dma((groups - 1, 2)),
            dma((chunks // 2,)),
            dma,
            dma((groups - 1, chunks // 2)),
            dma((2,)),
            dma((3,)),
            regular,
            regular((2,)),
        ],
        compiler_params=pltpu.CompilerParams(
            collective_id=0, has_side_effects=True, vmem_limit_bytes=48 * MIB
        ),
    )(*[pltpu.with_memory_space_constraint(x, pltpu.HBM) for x in (tridiag_vectors.T, ritz_values[None])], krylov_basis, krylov_image)
    return pl.pallas_call(
        finish_kernel,
        name="finish",
        out_shape=(out, out, jax.ShapeDtypeStruct((wanted_dev,), f32)),
        in_specs=[vmem] * 4,
        out_specs=(hbm, hbm, hbm),
        scratch_shapes=[
            pltpu.VMEM((2, wanted_dev, outer_dev, groups * inner_dev), f32),
            pltpu.VMEM((wanted_dev,), f32),
            dma((3,)),
        ],
        compiler_params=pltpu.CompilerParams(vmem_limit_bytes=16 * MIB),
    )(ritz, resid, factor, norms)


def solution(mesh):
    placed = (P(None, "row", "grp"), P(None, "row", "grp"), P(None, "grp"), P("grp"))
    return jax.shard_map(
        functools.partial(body, mesh.shape["grp"], mesh.shape["row"]),
        mesh=mesh,
        in_specs=placed,
        out_specs=(P("grp", "row", None), P("grp", "row", None), P("grp")),
        check_vma=False,
    )
```

```python
import functools
import math

import jax
import jax.numpy as jnp
from jax import lax
from jax.experimental import pallas as pl
from jax.experimental.pallas import tpu as pltpu
from jax.sharding import PartitionSpec as P

MESH = pl.DeviceIdType.MESH
MIB = 1 << 20
TILE = 8
STEP = 16
LANES = 128
POWER = 13
PEAK = 2.0 ** (126.0 / POWER)
SHIFT = 2.0**30
LEAST = 1e-36


def cdiv(a, b):
    return (a + b - 1) // b


def grid_iota(shape, dim):
    return lax.broadcasted_iota(jnp.int32, shape, dim)


def expand_rows(cols, width):
    return jnp.broadcast_to(cols, (cols.shape[0], width)).reshape(cols.shape[0], 1, width)


def encode(cols, inverse):
    y = cols * inverse
    y2 = y * y
    y4 = y2 * y2
    y8 = y4 * y4
    return (y8 * y4) * y


def decode(codes):
    size = jnp.exp2(jnp.log(jnp.abs(codes)) * (1.0 / (POWER * math.log(2.0))))
    return jnp.where(codes < 0.0, -size, size)


def exchange_kernel(
    groups, rows, rows_total,
    tridiag_ref, values_ref, basis_ref, image_ref,
    ritz_ref, resid_ref, factor_ref, norm_ref,
    coefs, values, fields, spread, expanded, coded, received,
    stat_send, stat_recv, square_send, square_recv,
    coef_load, coef_send, coef_recv, load_sem, send_sem, recv_sem, small_send, small_recv,
    ready_sem, order_sem,
):
    wanted_dev, krylov_len = tridiag_ref.shape
    chunks = fields.shape[0]
    pairs = chunks // 2
    padded_len = fields.shape[2]
    inner_dev = basis_ref.shape[2]
    steps = padded_len // STEP
    wide = STEP * TILE
    block = wanted_dev * TILE
    planes = rows // 2
    grp = lax.axis_index("grp")
    row = lax.axis_index("row")
    core = lax.rem(row, 2)
    plane = lax.div(row, 2)
    lead = core == 1

    def partner(mask):
        if mask == 0:
            return grp
        if mask == 1:
            return grp + 1 - 2 * lax.rem(grp, 2)
        if mask == 2:
            return lax.rem(grp + 2, groups)
        return groups - 1 - grp

    def device(mask, at_plane, at_core):
        return {"grp": partner(mask), "row": 2 * at_plane + at_core}

    def signal(sem, where):
        pl.semaphore_signal(sem, inc=1, device_id=where, device_id_type=MESH)

    barrier = pltpu.get_barrier_semaphore()
    for mask in (1, 2):
        signal(barrier, device(mask, plane, 1))

    coef_loads = [
        pltpu.make_async_copy(tridiag_ref, coefs.at[0], coef_load.at[0]),
        pltpu.make_async_copy(values_ref, values.at[0], coef_load.at[1]),
    ]
    for copy in coef_loads:
        copy.start()

    @pl.when(core == 0)
    def _():
        signal(barrier, device(0, plane, 1))

        def greet(ahead, carry):
            signal(barrier, device(0, lax.rem(plane + ahead, planes), 0))
            return carry

        lax.fori_loop(1, planes, greet, 0)

    for chunk in range(chunks):
        for which, ref in enumerate((basis_ref, image_ref)):
            pltpu.make_async_copy(
                ref.at[:, chunk * TILE : (chunk + 1) * TILE, :],
                fields.at[chunk, which, pl.ds(0, krylov_len)],
                load_sem.at[min(chunk // 2, 1)],
            ).start()

    def land(ref, sem):
        pltpu.make_async_copy(ref, ref, sem).wait()

    def load_wait(start, count):
        land(fields.at[pl.ds(start, count), :, pl.ds(0, krylov_len)], load_sem.at[min(start, 1)])

    if padded_len > krylov_len:
        for chunk in range(chunks):
            for which in range(2):
                fields[chunk, which, pl.ds(krylov_len, padded_len - krylov_len)] = jnp.zeros(
                    (padded_len - krylov_len, TILE, inner_dev), jnp.bfloat16
                )
    shape = spread.shape
    spread[...] = jnp.where(
        lax.shift_right_logical(grid_iota(shape, 1), 3) == grid_iota(shape, 0), SHIFT, 0.0
    ).astype(jnp.bfloat16)

    for copy in coef_loads:
        copy.wait()

    def coef_copies(source, slot, mask, at_core):
        return [
            pltpu.make_async_remote_copy(
                src_ref=ref.at[source],
                dst_ref=ref.at[slot],
                send_sem=coef_send.at[kind],
                recv_sem=coef_recv.at[slot - 1, kind],
                device_id=device(mask, plane, at_core),
                device_id_type=MESH,
            )
            for kind, ref in enumerate((coefs, values))
        ]

    own_sends = [
        copy
        for mask in (1, 2)
        for at_core in (1, 0)
        for copy in coef_copies(0, mask, mask, at_core)
    ]
    relay_sends = [copy for at_core in (1, 0) for copy in coef_copies(1, 3, 2, at_core)]

    def coef_wait(slot):
        for copy in coef_copies(0, slot, 1, 1):
            copy.wait_recv()

    @pl.when(lead)
    def _():
        pl.semaphore_wait(barrier, 5)
        for copy in own_sends:
            copy.start()
        signal(ready_sem, device(0, plane, 0))
        coef_wait(1)
        for copy in relay_sends:
            copy.start()
        coef_wait(2)

    @pl.when(core == 0)
    def _():
        pl.semaphore_wait(ready_sem, 1)
        coef_wait(1)
        coef_wait(2)

    near = grid_iota((wanted_dev, wanted_dev), 0) == grid_iota((wanted_dev, wanted_dev), 1)
    same = (grid_iota((TILE, wide), 1) & (TILE - 1)) == grid_iota((TILE, wide), 0)
    per_part = LANES // STEP
    pair = 2 * wanted_dev
    lane = grid_iota((pair, LANES), 1)

    def prepare(slots):
        shifts = []
        for slot in slots:
            spot = jnp.broadcast_to(values[slot].astype(jnp.float32), (wanted_dev, wanted_dev))
            shifts.append(jnp.sum(jnp.where(near, spot, 0.0), axis=1, keepdims=True))
        shift_values = expand_rows(jnp.concatenate(shifts, axis=0), inner_dev)
        both = jnp.concatenate([coefs[slot] for slot in slots], axis=0)
        for part in range(cdiv(krylov_len, LANES)):
            piece = both[:, part * LANES : min((part + 1) * LANES, krylov_len)]
            wider = jnp.dot(piece, spread[: piece.shape[1]], preferred_element_type=jnp.float32)
            for step in range(part * per_part, min((part + 1) * per_part, steps)):
                at = (step % per_part) * wide
                spot = jnp.where(same[None], wider[:, at : at + wide].reshape(pair, 1, wide), 0.0)
                expanded[:, step * wide : (step + 1) * wide] = spot.reshape(pair * TILE, wide).astype(jnp.bfloat16)
        return shift_values

    def compute(slots, shift_values, start, count, stats):
        both = jnp.concatenate(
            [
                fields[start + more, which].reshape(padded_len * TILE, inner_dev)
                for more in range(count)
                for which in range(2)
            ],
            axis=1,
        )
        product = jnp.dot(expanded[...], both, preferred_element_type=jnp.float32)
        product = product.reshape(pair, TILE, 2 * count * inner_dev)
        for more in range(count):
            chunk = start + more
            at = 2 * more * inner_dev
            ritz = product[:, :, at : at + inner_dev]
            resid = product[:, :, at + inner_dev : at + 2 * inner_dev] - shift_values * ritz
            for kind, cols in enumerate((ritz, resid)):
                squares = jnp.sum(jnp.sum(cols * cols, axis=1), axis=1, keepdims=True)
                stats = jnp.where(lane == 2 * chunk + kind, squares, stats)
                inverse = expand_rows(PEAK / jnp.sqrt(jnp.maximum(squares, LEAST)), inner_dev)
                for index, slot in enumerate(slots):
                    part = slice(index * wanted_dev, (index + 1) * wanted_dev)
                    if slot == 0:
                        put_out(kind, chunk, grp, cols[part])
                    else:
                        coded[slot - 1, chunk, :, kind * inner_dev : (kind + 1) * inner_dev] = encode(
                            cols[part], inverse[part]
                        ).reshape(block, inner_dev).astype(jnp.bfloat16)
        return stats

    def put_out(kind, chunk, source, cols):
        span = pl.ds(pl.multiple_of(chunk * TILE, TILE), TILE)
        lanes = pl.ds(pl.multiple_of(source * inner_dev, inner_dev), inner_dev)
        (ritz_ref, resid_ref)[kind][:, span, lanes] = cols

    def data_copy(mask, start, final=0):
        span = pl.ds(start, 2)
        return pltpu.make_async_remote_copy(
            src_ref=coded.at[mask - 1, span],
            dst_ref=received.at[mask - 1, span],
            send_sem=send_sem,
            recv_sem=recv_sem.at[mask - 1, final],
            device_id=device(mask, plane, core),
            device_id_type=MESH,
        )

    def stat_copy(mask):
        return pltpu.make_async_remote_copy(
            src_ref=stat_send.at[mask],
            dst_ref=stat_recv.at[mask],
            send_sem=small_send.at[0],
            recv_sem=small_recv.at[0 if mask < 3 else 2],
            device_id=device(mask, plane, core),
            device_id_type=MESH,
        )

    def squares_to(mask, at_plane, flip):
        pltpu.make_async_remote_copy(
            src_ref=square_send.at[mask],
            dst_ref=square_recv.at[grp * rows + row],
            send_sem=small_send.at[1],
            recv_sem=small_recv.at[1],
            device_id=device(mask, at_plane, lax.rem(core + flip, 2)),
            device_id_type=MESH,
        ).start()

    def far_squares(at_plane, carry):
        for mask in range(groups):
            for flip in range(2):
                squares_to(mask, at_plane, flip)
        return carry

    def agree(side, count):
        @pl.when(core == 0)
        def _():
            pl.semaphore_wait(order_sem.at[side], count)
            signal(order_sem.at[side], device(0, plane, 1))

        @pl.when(lead)
        def _():
            pl.semaphore_wait(order_sem.at[side], 1)

    def finish_stats(slots, stats):
        parity = lane & 1
        column = lax.rem(grid_iota((pair, LANES), 0), wanted_dev)
        line = jnp.zeros((pair, LANES), jnp.float32)
        for kind in range(2):
            sums = jnp.sum(jnp.where(parity == kind, stats, 0.0), axis=1, keepdims=True)
            line = jnp.where(lane == column + kind * wanted_dev, sums, line)
        scales = jnp.sqrt(jnp.maximum(stats, LEAST))
        for index, slot in enumerate(slots):
            part = slice(index * wanted_dev, (index + 1) * wanted_dev)
            square_send[slot] = jnp.sum(line[part], axis=0, keepdims=True)
            if slot:
                stat_send[slot] = scales[part]

    nothing = jnp.zeros((pair, LANES), jnp.float32)
    load_wait(0, 2)
    shift_values = prepare((1, 2))
    stats = compute((1, 2), shift_values, 0, 2, nothing)
    for mask in (2, 1):
        data_copy(mask, 0).start()
    load_wait(2, chunks - 2)
    def first(step, stats):
        stats = compute((1, 2), shift_values, 2 * step, 2, stats)
        @pl.when(step < pairs - 1)
        def _():
            for mask in (1, 2):
                data_copy(mask, 2 * step).start()

        return stats

    stats = lax.fori_loop(1, pairs, first, stats)
    finish_stats((1, 2), stats)
    for mask in (1, 2):
        stat_copy(mask).start()

    @pl.when(core == 0)
    def _():
        data_copy(2, chunks - 2, 1).start()


    coef_wait(3)
    if planes > 1:
        @pl.when(core == 0)
        def _():
            pl.semaphore_wait(barrier, planes - 1)

            def lower(other, carry):
                signal(order_sem.at[1], device(0, other, 0))
                return carry

            def upper(other, carry):
                signal(order_sem.at[0], device(0, other, 0))
                return carry

            lax.fori_loop(plane + 1, planes, upper, 0)
            lax.fori_loop(0, plane, lower, 0)

    shift_other = prepare((3, 0))

    def second(step, stats):
        stats = compute((3, 0), shift_other, 2 * step, 2, stats)

        @pl.when(lax.rem(step, 2) == 0)
        def _():
            data_copy(3, step).start()

        return stats

    stats = lax.fori_loop(0, pairs, second, nothing)
    finish_stats((3, 0), stats)

    stat_copy(3).start()
    for mask in range(groups):
        for flip in range(0 if mask else 1, 2):
            squares_to(mask, plane, flip)
    if planes > 1:
        @pl.when(plane > 0)
        def _():
            agree(0, plane)
            lax.fori_loop(0, plane, far_squares, 0)

    def across(step, carry):
        data_copy(3, 2 * step).start()
        return carry

    lax.fori_loop(cdiv(pairs, 2), pairs - 1, across, 0)
    data_copy(3, chunks - 2, 1).start()

    @pl.when(core == 0)
    def _():
        data_copy(1, chunks - 2, 1).start()


    if planes > 1:
        @pl.when(plane < planes - 1)
        def _():
            agree(1, planes - 1 - plane)
            lax.fori_loop(plane + 1, planes, far_squares, 0)

    land(stat_recv.at[pl.ds(1, 2)], small_recv.at[0])

    lane_dev = grid_iota((wanted_dev, LANES), 1)

    def arrive(mask, final):
        span = pl.ds(chunks - 2, 2) if final else pl.ds(0, chunks - 2)
        land(received.at[mask - 1, span], recv_sem.at[mask - 1, final])

    def take(masks, step, carry):
        for half in range(2):
            chunk = 2 * step + half
            for mask in masks:
                for kind in range(2):
                    scale = jnp.sum(
                        jnp.where(lane_dev == 2 * chunk + kind, stat_recv[mask], 0.0), axis=1, keepdims=True
                    )
                    codes = received[mask - 1, chunk, :, kind * inner_dev : (kind + 1) * inner_dev]
                    size = decode(codes.astype(jnp.float32)).reshape(wanted_dev, TILE, inner_dev)
                    put_out(kind, chunk, partner(mask), size * expand_rows(scale * (1.0 / PEAK), inner_dev))
        return carry

    for mask in (1, 2):
        arrive(mask, 0)

    @pl.when(lead)
    def _():
        data_copy(2, chunks - 2, 1).start()
        data_copy(1, chunks - 2, 1).start()

    lax.fori_loop(0, pairs - 1, functools.partial(take, (1, 2)), 0)
    land(stat_recv.at[3], small_recv.at[2])
    arrive(3, 0)
    lax.fori_loop(0, pairs - 1, functools.partial(take, (3,)), 0)
    arrive(2, 1)
    take((2,), pairs - 1, 0)

    others = groups * rows - 1
    land(square_recv.at[pl.ds(0, others)], small_recv.at[1])
    square_recv[grp * rows + row] = square_send[0]
    total = jnp.broadcast_to(jnp.sum(square_recv[...], axis=0), (wanted_dev, LANES))
    column = grid_iota((wanted_dev, LANES), 0)
    unit = 1.0 / (SHIFT * SHIFT)
    ritz_squares, resid_squares = (
        jnp.sum(jnp.where(lane_dev == column + kind * wanted_dev, total, 0.0), axis=1, keepdims=True) * unit
        for kind in range(2)
    )
    ritz_squares = ritz_squares + 1.0
    factor_ref[...] = jnp.broadcast_to(
        jnp.sqrt(rows_total / ritz_squares) * (1.0 / SHIFT), (wanted_dev, LANES)
    )
    norms = jnp.broadcast_to(jnp.sqrt(resid_squares / ritz_squares), (wanted_dev, LANES))
    norm_ref[...] = jnp.sum(jnp.where(lane_dev == column, norms, 0.0), axis=0, keepdims=True)

    land(square_recv.at[pl.ds(0, others)], small_send.at[1])
    land(stat_send.at[pl.ds(1, groups - 1)], small_send.at[0])

    @pl.when(lead)
    def _():
        for kind, ref in enumerate((coefs, values)):
            land(ref, coef_send.at[kind])

    arrive(3, 1)
    take((3,), pairs - 1, 0)
    arrive(1, 1)
    take((1,), pairs - 1, 0)
    land(coded, send_sem)


def finish_kernel(ritz_in, resid_in, factor_ref, norm_in, ritz_out, resid_out, norm_out, scaled, norm, sems):
    wanted_dev, _, inner = ritz_in.shape
    norm[...] = norm_in[0, :wanted_dev]
    norm_copy = pltpu.make_async_copy(norm, norm_out, sems.at[2])
    norm_copy.start()
    for column in range(wanted_dev):
        span = slice(column, column + 1)
        spot = jnp.broadcast_to(factor_ref[span], (TILE, LANES))
        spot = jnp.concatenate([spot] * (inner // LANES), axis=1)[None]
        for kind, (source, out) in enumerate(((ritz_in, ritz_out), (resid_in, resid_out))):
            for at in range(0, source.shape[1], TILE):
                scaled[kind, span, at : at + TILE] = source[span, at : at + TILE] * spot
            pltpu.make_async_copy(scaled.at[kind, span], out.at[span], sems.at[kind]).start()
    norm_copy.wait()
    for kind, out in enumerate((ritz_out, resid_out)):
        pltpu.make_async_copy(scaled.at[kind], out, sems.at[kind]).wait()


def body(groups, rows, krylov_basis, krylov_image, tridiag_vectors, ritz_values):
    krylov_len, outer_dev, inner_dev = krylov_basis.shape
    wanted_dev = tridiag_vectors.shape[1]
    chunks = outer_dev // TILE
    block = wanted_dev * TILE
    planes = rows // 2
    assert groups == 4 and rows == 2 * planes and chunks % 2 == 0
    padded_len = cdiv(krylov_len, STEP) * STEP
    rows_total = float(outer_dev * inner_dev * groups * rows)
    f32, bf16 = jnp.float32, jnp.bfloat16
    dma, regular = pltpu.SemaphoreType.DMA, pltpu.SemaphoreType.REGULAR
    vmem = pl.BlockSpec(memory_space=pltpu.VMEM)
    hbm = pl.BlockSpec(memory_space=pltpu.HBM)
    out = jax.ShapeDtypeStruct((wanted_dev, outer_dev, groups * inner_dev), f32)
    ritz, resid, factor, norms = pl.pallas_call(
        functools.partial(exchange_kernel, groups, rows, rows_total),
        name="exchange",
        out_shape=(
            out, out, jax.ShapeDtypeStruct((wanted_dev, LANES), f32), jax.ShapeDtypeStruct((1, LANES), f32),
        ),
        in_specs=[hbm] * 4,
        out_specs=(vmem,) * 4,
        scratch_shapes=[
            pltpu.VMEM((6, wanted_dev, krylov_len), bf16),
            pltpu.VMEM((6, 1, wanted_dev), bf16),
            pltpu.VMEM((chunks, 2, padded_len, TILE, inner_dev), bf16),
            pltpu.VMEM((LANES, LANES * TILE), bf16),
            pltpu.VMEM((2 * wanted_dev * TILE, padded_len * TILE), bf16),
            pltpu.VMEM((groups - 1, chunks, block, 2 * inner_dev), bf16),
            pltpu.VMEM((groups - 1, chunks, block, 2 * inner_dev), bf16),
            pltpu.VMEM((groups, wanted_dev, LANES), f32),
            pltpu.VMEM((groups, wanted_dev, LANES), f32),
            pltpu.VMEM((groups, 1, LANES), f32),
            pltpu.VMEM((groups * rows, 1, LANES), f32),
            dma((2,)),
            dma((2,)),
            dma((groups - 1, 2)),
            dma((2,)),
            dma,
            dma((groups - 1, 2)),
            dma((2,)),
            dma((3,)),
            regular,
            regular((2,)),
        ],
        compiler_params=pltpu.CompilerParams(
            collective_id=0, has_side_effects=True, vmem_limit_bytes=48 * MIB
        ),
    )(*[pltpu.with_memory_space_constraint(x, pltpu.HBM) for x in (tridiag_vectors.T, ritz_values[None])], krylov_basis, krylov_image)
    return pl.pallas_call(
        finish_kernel,
        name="finish",
        out_shape=(out, out, jax.ShapeDtypeStruct((wanted_dev,), f32)),
        in_specs=[vmem] * 4,
        out_specs=(hbm, hbm, hbm),
        scratch_shapes=[
            pltpu.VMEM((2, wanted_dev, outer_dev, groups * inner_dev), f32),
            pltpu.VMEM((wanted_dev,), f32),
            dma((3,)),
        ],
        compiler_params=pltpu.CompilerParams(vmem_limit_bytes=16 * MIB),
    )(ritz, resid, factor, norms)


def solution(mesh):
    placed = (P(None, "row", "grp"), P(None, "row", "grp"), P(None, "grp"), P("grp"))
    return jax.shard_map(
        functools.partial(body, mesh.shape["grp"], mesh.shape["row"]),
        mesh=mesh,
        in_specs=placed,
        out_specs=(P("grp", "row", None), P("grp", "row", None), P("grp")),
        check_vma=False,
    )
```

```python
import functools
import math

import jax
import jax.numpy as jnp
from jax import lax
from jax.experimental import pallas as pl
from jax.experimental.pallas import tpu as pltpu
from jax.sharding import PartitionSpec as P

MESH = pl.DeviceIdType.MESH
MIB = 1 << 20
TILE = 8
STEP = 16
LANES = 128
POWER = 13
PEAK = 2.0 ** (126.0 / POWER)
SHIFT = 2.0**30
LEAST = 1e-36


def cdiv(a, b):
    return (a + b - 1) // b


def grid_iota(shape, dim):
    return lax.broadcasted_iota(jnp.int32, shape, dim)


def expand_rows(cols, width):
    return jnp.broadcast_to(cols, (cols.shape[0], width)).reshape(cols.shape[0], 1, width)


def encode(cols, inverse):
    y = cols * inverse
    y2 = y * y
    y4 = y2 * y2
    y8 = y4 * y4
    return (y8 * y4) * y


def decode(codes):
    size = jnp.exp2(jnp.log(jnp.abs(codes)) * (1.0 / (POWER * math.log(2.0))))
    return jnp.where(codes < 0.0, -size, size)


def exchange_kernel(
    groups, rows, rows_total,
    tridiag_ref, values_ref, basis_ref, image_ref,
    ritz_ref, resid_ref, factor_ref, norm_ref,
    coefs, values, fields, spread, expanded, coded, received,
    stat_send, stat_recv, square_send, square_recv,
    coef_load, coef_send, coef_recv, load_sem, send_sem, recv_sem, small_send, small_recv,
    ready_sem, order_sem,
):
    wanted_dev, krylov_len = tridiag_ref.shape
    chunks = fields.shape[0]
    pairs = chunks // 2
    padded_len = fields.shape[2]
    inner_dev = basis_ref.shape[2]
    steps = padded_len // STEP
    wide = STEP * TILE
    block = wanted_dev * TILE
    planes = rows // 2
    grp = lax.axis_index("grp")
    row = lax.axis_index("row")
    core = lax.rem(row, 2)
    plane = lax.div(row, 2)
    lead = core == 1
    last_group = jnp.where(grp == groups - 1, 1, 0)

    def partner(mask):
        if mask == 0:
            return grp
        if mask == 1:
            return grp + 1 - 2 * lax.rem(grp, 2)
        if mask == 2:
            return lax.rem(grp + 2, groups)
        return groups - 1 - grp

    def device(mask, at_plane, at_core):
        return {"grp": partner(mask), "row": 2 * at_plane + at_core}

    def signal(sem, where):
        pl.semaphore_signal(sem, inc=1, device_id=where, device_id_type=MESH)

    barrier = pltpu.get_barrier_semaphore()
    for mask in (1, 2):
        signal(barrier, device(mask, plane, 1))

    coef_loads = [
        pltpu.make_async_copy(tridiag_ref, coefs.at[0], coef_load.at[0]),
        pltpu.make_async_copy(values_ref, values.at[0], coef_load.at[1]),
    ]
    for copy in coef_loads:
        copy.start()

    @pl.when(core == 0)
    def _():
        signal(barrier, device(0, plane, 1))

        def greet(ahead, carry):
            signal(barrier, device(0, lax.rem(plane + ahead, planes), 0))
            return carry

        lax.fori_loop(1, planes, greet, 0)

    for chunk in range(chunks):
        for which, ref in enumerate((basis_ref, image_ref)):
            pltpu.make_async_copy(
                ref.at[:, chunk * TILE : (chunk + 1) * TILE, :],
                fields.at[chunk, which, pl.ds(0, krylov_len)],
                load_sem.at[min(chunk // 2, 1)],
            ).start()

    def land(ref, sem):
        pltpu.make_async_copy(ref, ref, sem).wait()

    def load_wait(start, count):
        land(fields.at[pl.ds(start, count), :, pl.ds(0, krylov_len)], load_sem.at[min(start, 1)])

    if padded_len > krylov_len:
        for chunk in range(chunks):
            for which in range(2):
                fields[chunk, which, pl.ds(krylov_len, padded_len - krylov_len)] = jnp.zeros(
                    (padded_len - krylov_len, TILE, inner_dev), jnp.bfloat16
                )
    shape = spread.shape
    spread[...] = jnp.where(
        lax.shift_right_logical(grid_iota(shape, 1), 3) == grid_iota(shape, 0), SHIFT, 0.0
    ).astype(jnp.bfloat16)

    for copy in coef_loads:
        copy.wait()

    def coef_copies(source, slot, mask, at_core):
        return [
            pltpu.make_async_remote_copy(
                src_ref=ref.at[source],
                dst_ref=ref.at[slot],
                send_sem=coef_send.at[kind],
                recv_sem=coef_recv.at[slot - 1, kind],
                device_id=device(mask, plane, at_core),
                device_id_type=MESH,
            )
            for kind, ref in enumerate((coefs, values))
        ]

    own_sends = [
        copy
        for mask in (1, 2)
        for at_core in (1, 0)
        for copy in coef_copies(0, mask, mask, at_core)
    ]
    relay_sends = [copy for at_core in (1, 0) for copy in coef_copies(1, 3, 2, at_core)]

    def coef_wait(slot):
        for copy in coef_copies(0, slot, 1, 1):
            copy.wait_recv()

    @pl.when(lead)
    def _():
        pl.semaphore_wait(barrier, 5)
        for copy in own_sends:
            copy.start()
        signal(ready_sem, device(0, plane, 0))
        coef_wait(1)
        for copy in relay_sends:
            copy.start()
        coef_wait(2)

    @pl.when(core == 0)
    def _():
        pl.semaphore_wait(ready_sem, 1)
        coef_wait(1)
        coef_wait(2)

    near = grid_iota((wanted_dev, wanted_dev), 0) == grid_iota((wanted_dev, wanted_dev), 1)
    same = (grid_iota((TILE, wide), 1) & (TILE - 1)) == grid_iota((TILE, wide), 0)
    per_part = LANES // STEP
    pair = 2 * wanted_dev
    lane = grid_iota((pair, LANES), 1)

    def prepare(slots):
        shifts = []
        for slot in slots:
            spot = jnp.broadcast_to(values[slot].astype(jnp.float32), (wanted_dev, wanted_dev))
            shifts.append(jnp.sum(jnp.where(near, spot, 0.0), axis=1, keepdims=True))
        shift_values = expand_rows(jnp.concatenate(shifts, axis=0), inner_dev)
        both = jnp.concatenate([coefs[slot] for slot in slots], axis=0)
        for part in range(cdiv(krylov_len, LANES)):
            piece = both[:, part * LANES : min((part + 1) * LANES, krylov_len)]
            wider = jnp.dot(piece, spread[: piece.shape[1]], preferred_element_type=jnp.float32)
            for step in range(part * per_part, min((part + 1) * per_part, steps)):
                at = (step % per_part) * wide
                spot = jnp.where(same[None], wider[:, at : at + wide].reshape(pair, 1, wide), 0.0)
                expanded[:, step * wide : (step + 1) * wide] = spot.reshape(pair * TILE, wide).astype(jnp.bfloat16)
        return shift_values

    def compute(slots, shift_values, start, count, stats, after=None):
        both = jnp.concatenate(
            [
                fields[start + more, which].reshape(padded_len * TILE, inner_dev)
                for more in range(count)
                for which in range(2)
            ],
            axis=1,
        )
        product = jnp.dot(expanded[...], both, preferred_element_type=jnp.float32)
        product = product.reshape(pair, TILE, 2 * count * inner_dev)
        for more in range(count):
            chunk = start + more
            at = 2 * more * inner_dev
            ritz = product[:, :, at : at + inner_dev]
            resid = product[:, :, at + inner_dev : at + 2 * inner_dev] - shift_values * ritz
            for kind, cols in enumerate((ritz, resid)):
                squares = jnp.sum(jnp.sum(cols * cols, axis=1), axis=1, keepdims=True)
                stats = jnp.where(lane == 2 * chunk + kind, squares, stats)
                inverse = expand_rows(PEAK / jnp.sqrt(jnp.maximum(squares, LEAST)), inner_dev)
                for index, slot in enumerate(slots):
                    part = slice(index * wanted_dev, (index + 1) * wanted_dev)
                    if slot == 0:
                        put_out(kind, chunk, grp, cols[part])
                    else:
                        coded[slot - 1, chunk, :, kind * inner_dev : (kind + 1) * inner_dev] = encode(
                            cols[part], inverse[part]
                        ).reshape(block, inner_dev).astype(jnp.bfloat16)
            if after is not None:
                after(chunk)
        return stats

    def put_out(kind, chunk, source, cols):
        span = pl.ds(pl.multiple_of(chunk * TILE, TILE), TILE)
        lanes = pl.ds(pl.multiple_of(source * inner_dev, inner_dev), inner_dev)
        (ritz_ref, resid_ref)[kind][:, span, lanes] = cols

    def data_copy(mask, start, final=0, count=2):
        span = pl.ds(start, count)
        return pltpu.make_async_remote_copy(
            src_ref=coded.at[mask - 1, span],
            dst_ref=received.at[mask - 1, span],
            send_sem=send_sem,
            recv_sem=recv_sem.at[mask - 1, final],
            device_id=device(mask, plane, core),
            device_id_type=MESH,
        )

    def stat_copy(mask):
        return pltpu.make_async_remote_copy(
            src_ref=stat_send.at[mask],
            dst_ref=stat_recv.at[mask],
            send_sem=small_send.at[0],
            recv_sem=small_recv.at[0 if mask < 3 else 2],
            device_id=device(mask, plane, core),
            device_id_type=MESH,
        )

    def squares_to(mask, at_plane, flip):
        pltpu.make_async_remote_copy(
            src_ref=square_send.at[mask],
            dst_ref=square_recv.at[grp * rows + row],
            send_sem=small_send.at[1],
            recv_sem=small_recv.at[1],
            device_id=device(mask, at_plane, lax.rem(core + flip, 2)),
            device_id_type=MESH,
        ).start()

    def far_squares(at_plane, carry):
        for mask in range(groups):
            for flip in range(2):
                squares_to(mask, at_plane, flip)
        return carry

    def agree(side, count):
        @pl.when(core == 0)
        def _():
            pl.semaphore_wait(order_sem.at[side], count)
            signal(order_sem.at[side], device(0, plane, 1))

        @pl.when(lead)
        def _():
            pl.semaphore_wait(order_sem.at[side], 1)

    def finish_stats(slots, stats):
        parity = lane & 1
        column = lax.rem(grid_iota((pair, LANES), 0), wanted_dev)
        line = jnp.zeros((pair, LANES), jnp.float32)
        for kind in range(2):
            sums = jnp.sum(jnp.where(parity == kind, stats, 0.0), axis=1, keepdims=True)
            line = jnp.where(lane == column + kind * wanted_dev, sums, line)
        scales = jnp.sqrt(jnp.maximum(stats, LEAST))
        for index, slot in enumerate(slots):
            part = slice(index * wanted_dev, (index + 1) * wanted_dev)
            square_send[slot] = jnp.sum(line[part], axis=0, keepdims=True)
            if slot:
                stat_send[slot] = scales[part]

    nothing = jnp.zeros((pair, LANES), jnp.float32)
    load_wait(0, 2)
    shift_values = prepare((1, 2))

    def send_chunk(chunk):
        for mask in (2, 1):
            data_copy(mask, chunk, count=1).start()

    stats = compute((1, 2), shift_values, 0, 2, nothing, send_chunk)
    load_wait(2, chunks - 2)
    def first(step, stats):
        stats = compute((1, 2), shift_values, 2 * step, 2, stats)
        @pl.when(step < pairs - 1)
        def _():
            data_copy(2, 2 * step).start()

        @pl.when(step < pairs - 1 - last_group)
        def _():
            data_copy(1, 2 * step).start()

        return stats

    stats = lax.fori_loop(1, pairs, first, stats)
    finish_stats((1, 2), stats)
    for mask in (1, 2):
        stat_copy(mask).start()

    @pl.when(core == 0)
    def _():
        data_copy(2, chunks - 2, 1).start()


    coef_wait(3)
    if planes > 1:
        @pl.when(core == 0)
        def _():
            pl.semaphore_wait(barrier, planes - 1)

            def lower(other, carry):
                signal(order_sem.at[1], device(0, other, 0))
                return carry

            def upper(other, carry):
                signal(order_sem.at[0], device(0, other, 0))
                return carry

            lax.fori_loop(plane + 1, planes, upper, 0)
            lax.fori_loop(0, plane, lower, 0)

    shift_other = prepare((3, 0))

    def second(step, stats):
        stats = compute((3, 0), shift_other, 2 * step, 2, stats)

        @pl.when(jnp.logical_and(last_group == 0, lax.rem(step, 2) == 0))
        def _():
            data_copy(3, step).start()

        @pl.when(jnp.logical_and(last_group == 1, step < pairs - 1))
        def _():
            data_copy(3, 2 * step).start()

        return stats

    stats = lax.fori_loop(0, pairs, second, nothing)
    finish_stats((3, 0), stats)

    stat_copy(3).start()
    for mask in range(groups):
        for flip in range(0 if mask else 1, 2):
            squares_to(mask, plane, flip)
    if planes > 1:
        @pl.when(plane > 0)
        def _():
            agree(0, plane)
            lax.fori_loop(0, plane, far_squares, 0)

    def across(step, carry):
        data_copy(3, 2 * step).start()
        return carry

    lax.fori_loop(jnp.where(last_group == 1, pairs - 1, cdiv(pairs, 2)), pairs - 1, across, 0)
    data_copy(3, chunks - 2, 1).start()

    @pl.when(last_group == 1)
    def _():
        data_copy(1, chunks - 4).start()


    @pl.when(core == 0)
    def _():
        data_copy(1, chunks - 2, 1).start()


    if planes > 1:
        @pl.when(plane < planes - 1)
        def _():
            agree(1, planes - 1 - plane)
            lax.fori_loop(plane + 1, planes, far_squares, 0)

    @pl.when(lead)
    def _():
        data_copy(2, chunks - 2, 1).start()
        data_copy(1, chunks - 2, 1).start()

    land(stat_recv.at[pl.ds(1, 2)], small_recv.at[0])

    lane_dev = grid_iota((wanted_dev, LANES), 1)

    def arrive(mask, final):
        span = pl.ds(chunks - 2, 2) if final else pl.ds(0, chunks - 2)
        land(received.at[mask - 1, span], recv_sem.at[mask - 1, final])

    def take(masks, step, carry):
        for half in range(2):
            chunk = 2 * step + half
            for mask in masks:
                for kind in range(2):
                    scale = jnp.sum(
                        jnp.where(lane_dev == 2 * chunk + kind, stat_recv[mask], 0.0), axis=1, keepdims=True
                    )
                    codes = received[mask - 1, chunk, :, kind * inner_dev : (kind + 1) * inner_dev]
                    size = decode(codes.astype(jnp.float32)).reshape(wanted_dev, TILE, inner_dev)
                    put_out(kind, chunk, partner(mask), size * expand_rows(scale * (1.0 / PEAK), inner_dev))
        return carry

    arrive(2, 0)

    arrive(1, 0)
    lax.fori_loop(0, pairs - 1, functools.partial(take, (1, 2)), 0)
    land(stat_recv.at[3], small_recv.at[2])
    arrive(3, 0)
    lax.fori_loop(0, pairs - 1, functools.partial(take, (3,)), 0)
    arrive(2, 1)
    take((2,), pairs - 1, 0)

    others = groups * rows - 1
    land(square_recv.at[pl.ds(0, others)], small_recv.at[1])
    square_recv[grp * rows + row] = square_send[0]
    total = jnp.broadcast_to(jnp.sum(square_recv[...], axis=0), (wanted_dev, LANES))
    column = grid_iota((wanted_dev, LANES), 0)
    unit = 1.0 / (SHIFT * SHIFT)
    ritz_squares, resid_squares = (
        jnp.sum(jnp.where(lane_dev == column + kind * wanted_dev, total, 0.0), axis=1, keepdims=True) * unit
        for kind in range(2)
    )
    ritz_squares = ritz_squares + 1.0
    factor_ref[...] = jnp.broadcast_to(
        jnp.sqrt(rows_total / ritz_squares) * (1.0 / SHIFT), (wanted_dev, LANES)
    )
    norms = jnp.broadcast_to(jnp.sqrt(resid_squares / ritz_squares), (wanted_dev, LANES))
    norm_ref[...] = jnp.sum(jnp.where(lane_dev == column, norms, 0.0), axis=0, keepdims=True)

    land(square_recv.at[pl.ds(0, others)], small_send.at[1])
    land(stat_send.at[pl.ds(1, groups - 1)], small_send.at[0])

    @pl.when(lead)
    def _():
        for kind, ref in enumerate((coefs, values)):
            land(ref, coef_send.at[kind])

    arrive(3, 1)
    take((3,), pairs - 1, 0)
    arrive(1, 1)
    take((1,), pairs - 1, 0)
    land(coded, send_sem)


def finish_kernel(ritz_in, resid_in, factor_ref, norm_in, ritz_out, resid_out, norm_out, scaled, norm, sems):
    wanted_dev, _, inner = ritz_in.shape
    norm[...] = norm_in[0, :wanted_dev]
    norm_copy = pltpu.make_async_copy(norm, norm_out, sems.at[2])
    norm_copy.start()
    for column in range(wanted_dev):
        span = slice(column, column + 1)
        spot = jnp.broadcast_to(factor_ref[span], (TILE, LANES))
        spot = jnp.concatenate([spot] * (inner // LANES), axis=1)[None]
        for kind, (source, out) in enumerate(((ritz_in, ritz_out), (resid_in, resid_out))):
            for at in range(0, source.shape[1], TILE):
                scaled[kind, span, at : at + TILE] = source[span, at : at + TILE] * spot
            pltpu.make_async_copy(scaled.at[kind, span], out.at[span], sems.at[kind]).start()
    norm_copy.wait()
    for kind, out in enumerate((ritz_out, resid_out)):
        pltpu.make_async_copy(scaled.at[kind], out, sems.at[kind]).wait()


def body(groups, rows, krylov_basis, krylov_image, tridiag_vectors, ritz_values):
    krylov_len, outer_dev, inner_dev = krylov_basis.shape
    wanted_dev = tridiag_vectors.shape[1]
    chunks = outer_dev // TILE
    block = wanted_dev * TILE
    planes = rows // 2
    assert groups == 4 and rows == 2 * planes and chunks % 2 == 0
    padded_len = cdiv(krylov_len, STEP) * STEP
    rows_total = float(outer_dev * inner_dev * groups * rows)
    f32, bf16 = jnp.float32, jnp.bfloat16
    dma, regular = pltpu.SemaphoreType.DMA, pltpu.SemaphoreType.REGULAR
    vmem = pl.BlockSpec(memory_space=pltpu.VMEM)
    hbm = pl.BlockSpec(memory_space=pltpu.HBM)
    out = jax.ShapeDtypeStruct((wanted_dev, outer_dev, groups * inner_dev), f32)
    ritz, resid, factor, norms = pl.pallas_call(
        functools.partial(exchange_kernel, groups, rows, rows_total),
        name="exchange",
        out_shape=(
            out, out, jax.ShapeDtypeStruct((wanted_dev, LANES), f32), jax.ShapeDtypeStruct((1, LANES), f32),
        ),
        in_specs=[hbm] * 4,
        out_specs=(vmem,) * 4,
        scratch_shapes=[
            pltpu.VMEM((6, wanted_dev, krylov_len), bf16),
            pltpu.VMEM((6, 1, wanted_dev), bf16),
            pltpu.VMEM((chunks, 2, padded_len, TILE, inner_dev), bf16),
            pltpu.VMEM((LANES, LANES * TILE), bf16),
            pltpu.VMEM((2 * wanted_dev * TILE, padded_len * TILE), bf16),
            pltpu.VMEM((groups - 1, chunks, block, 2 * inner_dev), bf16),
            pltpu.VMEM((groups - 1, chunks, block, 2 * inner_dev), bf16),
            pltpu.VMEM((groups, wanted_dev, LANES), f32),
            pltpu.VMEM((groups, wanted_dev, LANES), f32),
            pltpu.VMEM((groups, 1, LANES), f32),
            pltpu.VMEM((groups * rows, 1, LANES), f32),
            dma((2,)),
            dma((2,)),
            dma((groups - 1, 2)),
            dma((2,)),
            dma,
            dma((groups - 1, 2)),
            dma((2,)),
            dma((3,)),
            regular,
            regular((2,)),
        ],
        compiler_params=pltpu.CompilerParams(
            collective_id=0, has_side_effects=True, vmem_limit_bytes=48 * MIB
        ),
    )(*[pltpu.with_memory_space_constraint(x, pltpu.HBM) for x in (tridiag_vectors.T, ritz_values[None])], krylov_basis, krylov_image)
    return pl.pallas_call(
        finish_kernel,
        name="finish",
        out_shape=(out, out, jax.ShapeDtypeStruct((wanted_dev,), f32)),
        in_specs=[vmem] * 4,
        out_specs=(hbm, hbm, hbm),
        scratch_shapes=[
            pltpu.VMEM((2, wanted_dev, outer_dev, groups * inner_dev), f32),
            pltpu.VMEM((wanted_dev,), f32),
            dma((3,)),
        ],
        compiler_params=pltpu.CompilerParams(vmem_limit_bytes=16 * MIB),
    )(ritz, resid, factor, norms)


def solution(mesh):
    placed = (P(None, "row", "grp"), P(None, "row", "grp"), P(None, "grp"), P("grp"))
    return jax.shard_map(
        functools.partial(body, mesh.shape["grp"], mesh.shape["row"]),
        mesh=mesh,
        in_specs=placed,
        out_specs=(P("grp", "row", None), P("grp", "row", None), P("grp")),
        check_vma=False,
    )
```

```python
import functools
import math

import jax
import jax.numpy as jnp
from jax import lax
from jax.experimental import pallas as pl
from jax.experimental.pallas import tpu as pltpu
from jax.sharding import PartitionSpec as P

MESH = pl.DeviceIdType.MESH
MIB = 1 << 20
TILE = 8
STEP = 16
LANES = 128
POWER = 13
PEAK = 2.0 ** (126.0 / POWER)
SHIFT = 2.0**30
LEAST = 1e-36


def cdiv(a, b):
    return (a + b - 1) // b


def grid_iota(shape, dim):
    return lax.broadcasted_iota(jnp.int32, shape, dim)


def expand_rows(cols, width):
    return jnp.broadcast_to(cols, (cols.shape[0], width)).reshape(cols.shape[0], 1, width)


def encode(cols, inverse):
    y = cols * inverse
    y2 = y * y
    y4 = y2 * y2
    y8 = y4 * y4
    return (y8 * y4) * y


def decode(codes):
    size = jnp.exp2(jnp.log(jnp.abs(codes)) * (1.0 / (POWER * math.log(2.0))))
    return jnp.where(codes < 0.0, -size, size)


def exchange_kernel(
    groups, rows, rows_total,
    tridiag_ref, values_ref, basis_ref, image_ref,
    ritz_ref, resid_ref, factor_ref, norm_ref,
    coefs, values, fields, spread, expanded, coded, received,
    stat_send, stat_recv, square_send, square_recv,
    coef_load, coef_send, coef_recv, load_sem, send_sem, recv_sem, small_send, small_recv,
    ready_sem, order_sem,
):
    wanted_dev, krylov_len = tridiag_ref.shape
    chunks = fields.shape[0]
    pairs = chunks // 2
    padded_len = fields.shape[2]
    inner_dev = basis_ref.shape[2]
    steps = padded_len // STEP
    wide = STEP * TILE
    block = wanted_dev * TILE
    planes = rows // 2
    grp = lax.axis_index("grp")
    row = lax.axis_index("row")
    core = lax.rem(row, 2)
    plane = lax.div(row, 2)
    lead = core == 1
    last_group = jnp.where(grp == groups - 1, 1, 0)

    def partner(mask):
        if mask == 0:
            return grp
        if mask == 1:
            return grp + 1 - 2 * lax.rem(grp, 2)
        if mask == 2:
            return lax.rem(grp + 2, groups)
        return groups - 1 - grp

    def device(mask, at_plane, at_core):
        return {"grp": partner(mask), "row": 2 * at_plane + at_core}

    def signal(sem, where):
        pl.semaphore_signal(sem, inc=1, device_id=where, device_id_type=MESH)

    barrier = pltpu.get_barrier_semaphore()
    for mask in (1, 2):
        signal(barrier, device(mask, plane, 1))

    coef_loads = [
        pltpu.make_async_copy(tridiag_ref, coefs.at[0], coef_load.at[0]),
        pltpu.make_async_copy(values_ref, values.at[0], coef_load.at[1]),
    ]
    for copy in coef_loads:
        copy.start()

    @pl.when(core == 0)
    def _():
        signal(barrier, device(0, plane, 1))

        def greet(ahead, carry):
            signal(barrier, device(0, lax.rem(plane + ahead, planes), 0))
            return carry

        lax.fori_loop(1, planes, greet, 0)

    for chunk in range(chunks):
        for which, ref in enumerate((basis_ref, image_ref)):
            pltpu.make_async_copy(
                ref.at[:, chunk * TILE : (chunk + 1) * TILE, :],
                fields.at[chunk, which, pl.ds(0, krylov_len)],
                load_sem.at[min(chunk // 2, 1)],
            ).start()

    def land(ref, sem):
        pltpu.make_async_copy(ref, ref, sem).wait()

    def load_wait(start, count):
        land(fields.at[pl.ds(start, count), :, pl.ds(0, krylov_len)], load_sem.at[min(start, 1)])

    if padded_len > krylov_len:
        for chunk in range(chunks):
            for which in range(2):
                fields[chunk, which, pl.ds(krylov_len, padded_len - krylov_len)] = jnp.zeros(
                    (padded_len - krylov_len, TILE, inner_dev), jnp.bfloat16
                )
    shape = spread.shape
    spread[...] = jnp.where(
        lax.shift_right_logical(grid_iota(shape, 1), 3) == grid_iota(shape, 0), SHIFT, 0.0
    ).astype(jnp.bfloat16)

    for copy in coef_loads:
        copy.wait()

    def coef_copies(source, slot, mask, at_core):
        return [
            pltpu.make_async_remote_copy(
                src_ref=ref.at[source],
                dst_ref=ref.at[slot],
                send_sem=coef_send.at[kind],
                recv_sem=coef_recv.at[slot - 1, kind],
                device_id=device(mask, plane, at_core),
                device_id_type=MESH,
            )
            for kind, ref in enumerate((coefs, values))
        ]

    own_sends = [
        copy
        for mask in (1, 2)
        for at_core in (1, 0)
        for copy in coef_copies(0, mask, mask, at_core)
    ]
    relay_sends = [copy for at_core in (1, 0) for copy in coef_copies(1, 3, 2, at_core)]

    def coef_wait(slot):
        for copy in coef_copies(0, slot, 1, 1):
            copy.wait_recv()

    @pl.when(lead)
    def _():
        pl.semaphore_wait(barrier, 5)
        for copy in own_sends:
            copy.start()
        signal(ready_sem, device(0, plane, 0))
        coef_wait(1)
        for copy in relay_sends:
            copy.start()
        coef_wait(2)

    @pl.when(core == 0)
    def _():
        pl.semaphore_wait(ready_sem, 1)
        coef_wait(1)
        coef_wait(2)

    near = grid_iota((wanted_dev, wanted_dev), 0) == grid_iota((wanted_dev, wanted_dev), 1)
    same = (grid_iota((TILE, wide), 1) & (TILE - 1)) == grid_iota((TILE, wide), 0)
    per_part = LANES // STEP
    pair = 2 * wanted_dev
    lane = grid_iota((pair, LANES), 1)

    def prepare(slots):
        shifts = []
        for slot in slots:
            spot = jnp.broadcast_to(values[slot].astype(jnp.float32), (wanted_dev, wanted_dev))
            shifts.append(jnp.sum(jnp.where(near, spot, 0.0), axis=1, keepdims=True))
        shift_values = expand_rows(jnp.concatenate(shifts, axis=0), inner_dev)
        both = jnp.concatenate([coefs[slot] for slot in slots], axis=0)
        for part in range(cdiv(krylov_len, LANES)):
            piece = both[:, part * LANES : min((part + 1) * LANES, krylov_len)]
            wider = jnp.dot(piece, spread[: piece.shape[1]], preferred_element_type=jnp.float32)
            for step in range(part * per_part, min((part + 1) * per_part, steps)):
                at = (step % per_part) * wide
                spot = jnp.where(same[None], wider[:, at : at + wide].reshape(pair, 1, wide), 0.0)
                expanded[:, step * wide : (step + 1) * wide] = spot.reshape(pair * TILE, wide).astype(jnp.bfloat16)
        return shift_values

    def compute(slots, shift_values, start, count, stats, after=None):
        both = jnp.concatenate(
            [
                fields[start + more, which].reshape(padded_len * TILE, inner_dev)
                for more in range(count)
                for which in range(2)
            ],
            axis=1,
        )
        product = jnp.dot(expanded[...], both, preferred_element_type=jnp.float32)
        product = product.reshape(pair, TILE, 2 * count * inner_dev)
        for more in range(count):
            chunk = start + more
            at = 2 * more * inner_dev
            ritz = product[:, :, at : at + inner_dev]
            resid = product[:, :, at + inner_dev : at + 2 * inner_dev] - shift_values * ritz
            for kind, cols in enumerate((ritz, resid)):
                squares = jnp.sum(jnp.sum(cols * cols, axis=1), axis=1, keepdims=True)
                stats = jnp.where(lane == 2 * chunk + kind, squares, stats)
                inverse = expand_rows(PEAK / jnp.sqrt(jnp.maximum(squares, LEAST)), inner_dev)
                for index, slot in enumerate(slots):
                    part = slice(index * wanted_dev, (index + 1) * wanted_dev)
                    if slot == 0:
                        put_out(kind, chunk, grp, cols[part])
                    else:
                        coded[slot - 1, chunk, :, kind * inner_dev : (kind + 1) * inner_dev] = encode(
                            cols[part], inverse[part]
                        ).reshape(block, inner_dev).astype(jnp.bfloat16)
            if after is not None:
                after(chunk)
        return stats

    def put_out(kind, chunk, source, cols):
        span = pl.ds(pl.multiple_of(chunk * TILE, TILE), TILE)
        lanes = pl.ds(pl.multiple_of(source * inner_dev, inner_dev), inner_dev)
        (ritz_ref, resid_ref)[kind][:, span, lanes] = cols

    def data_copy(mask, start, final=0, count=2):
        span = pl.ds(start, count)
        return pltpu.make_async_remote_copy(
            src_ref=coded.at[mask - 1, span],
            dst_ref=received.at[mask - 1, span],
            send_sem=send_sem,
            recv_sem=recv_sem.at[mask - 1, final],
            device_id=device(mask, plane, core),
            device_id_type=MESH,
        )

    def stat_copy(mask):
        return pltpu.make_async_remote_copy(
            src_ref=stat_send.at[mask],
            dst_ref=stat_recv.at[mask],
            send_sem=small_send.at[0],
            recv_sem=small_recv.at[0 if mask < 3 else 2],
            device_id=device(mask, plane, core),
            device_id_type=MESH,
        )

    def squares_to(mask, at_plane, flip):
        pltpu.make_async_remote_copy(
            src_ref=square_send.at[mask],
            dst_ref=square_recv.at[grp * rows + row],
            send_sem=small_send.at[1],
            recv_sem=small_recv.at[1],
            device_id=device(mask, at_plane, lax.rem(core + flip, 2)),
            device_id_type=MESH,
        ).start()

    def far_squares(at_plane, carry):
        for mask in range(groups):
            for flip in range(2):
                squares_to(mask, at_plane, flip)
        return carry

    def agree(side, count):
        @pl.when(core == 0)
        def _():
            pl.semaphore_wait(order_sem.at[side], count)
            signal(order_sem.at[side], device(0, plane, 1))

        @pl.when(lead)
        def _():
            pl.semaphore_wait(order_sem.at[side], 1)

    def finish_stats(slots, stats):
        parity = lane & 1
        column = lax.rem(grid_iota((pair, LANES), 0), wanted_dev)
        line = jnp.zeros((pair, LANES), jnp.float32)
        for kind in range(2):
            sums = jnp.sum(jnp.where(parity == kind, stats, 0.0), axis=1, keepdims=True)
            line = jnp.where(lane == column + kind * wanted_dev, sums, line)
        scales = jnp.sqrt(jnp.maximum(stats, LEAST))
        for index, slot in enumerate(slots):
            part = slice(index * wanted_dev, (index + 1) * wanted_dev)
            square_send[slot] = jnp.sum(line[part], axis=0, keepdims=True)
            if slot:
                stat_send[slot] = scales[part]

    nothing = jnp.zeros((pair, LANES), jnp.float32)
    load_wait(0, 2)
    shift_values = prepare((1, 2))

    def send_chunk(chunk):
        for mask in (2, 1):
            data_copy(mask, chunk, count=1).start()

    stats = compute((1, 2), shift_values, 0, 2, nothing, send_chunk)
    load_wait(2, chunks - 2)
    def first(step, stats):
        stats = compute((1, 2), shift_values, 2 * step, 2, stats)
        @pl.when(step < pairs - 1)
        def _():
            data_copy(2, 2 * step).start()

        @pl.when(step < pairs - 1 - last_group)
        def _():
            data_copy(1, 2 * step).start()

        return stats

    stats = lax.fori_loop(1, pairs, first, stats)
    finish_stats((1, 2), stats)
    for mask in (1, 2):
        stat_copy(mask).start()

    @pl.when(core == 0)
    def _():
        data_copy(2, chunks - 2, 1).start()


    coef_wait(3)
    if planes > 1:
        @pl.when(core == 0)
        def _():
            pl.semaphore_wait(barrier, planes - 1)

            def lower(other, carry):
                signal(order_sem.at[1], device(0, other, 0))
                return carry

            def upper(other, carry):
                signal(order_sem.at[0], device(0, other, 0))
                return carry

            lax.fori_loop(plane + 1, planes, upper, 0)
            lax.fori_loop(0, plane, lower, 0)

    shift_other = prepare((3, 0))

    def second(step, stats):
        stats = compute((3, 0), shift_other, 2 * step, 2, stats)

        @pl.when(jnp.logical_and(last_group == 0, lax.rem(step, 2) == 0))
        def _():
            data_copy(3, step).start()

        @pl.when(jnp.logical_and(last_group == 1, step < pairs - 1))
        def _():
            data_copy(3, 2 * step).start()

        return stats

    stats = lax.fori_loop(0, pairs, second, nothing)
    finish_stats((3, 0), stats)

    stat_copy(3).start()
    for mask in range(groups):
        for flip in range(0 if mask else 1, 2):
            squares_to(mask, plane, flip)
    if planes > 1:
        @pl.when(plane > 0)
        def _():
            agree(0, plane)
            lax.fori_loop(0, plane, far_squares, 0)

    def across(step, carry):
        data_copy(3, 2 * step).start()
        return carry

    lax.fori_loop(jnp.where(last_group == 1, pairs - 1, cdiv(pairs, 2)), pairs - 1, across, 0)
    data_copy(3, chunks - 2, 1).start()

    @pl.when(last_group == 1)
    def _():
        data_copy(1, chunks - 4).start()


    @pl.when(core == 0)
    def _():
        data_copy(1, chunks - 2, 1).start()


    if planes > 1:
        @pl.when(plane < planes - 1)
        def _():
            agree(1, planes - 1 - plane)
            lax.fori_loop(plane + 1, planes, far_squares, 0)

    @pl.when(lead)
    def _():
        data_copy(2, chunks - 2, 1).start()
        data_copy(1, chunks - 2, 1).start()

    land(stat_recv.at[pl.ds(1, 2)], small_recv.at[0])

    lane_dev = grid_iota((wanted_dev, LANES), 1)

    def arrive(mask, final):
        span = pl.ds(chunks - 2, 2) if final else pl.ds(0, chunks - 2)
        land(received.at[mask - 1, span], recv_sem.at[mask - 1, final])

    def take(masks, step, carry):
        for half in range(2):
            chunk = 2 * step + half
            for mask in masks:
                for kind in range(2):
                    scale = jnp.sum(
                        jnp.where(lane_dev == 2 * chunk + kind, stat_recv[mask], 0.0), axis=1, keepdims=True
                    )
                    codes = received[mask - 1, chunk, :, kind * inner_dev : (kind + 1) * inner_dev]
                    size = decode(codes.astype(jnp.float32)).reshape(wanted_dev, TILE, inner_dev)
                    put_out(kind, chunk, partner(mask), size * expand_rows(scale * (1.0 / PEAK), inner_dev))
        return carry

    arrive(2, 0)

    arrive(1, 0)
    lax.fori_loop(0, pairs - 1, functools.partial(take, (1, 2)), 0)
    land(stat_recv.at[3], small_recv.at[2])
    arrive(3, 0)
    lax.fori_loop(0, pairs - 1, functools.partial(take, (3,)), 0)
    arrive(2, 1)
    take((2,), pairs - 1, 0)

    others = groups * rows - 1
    land(square_recv.at[pl.ds(0, others)], small_recv.at[1])
    square_recv[grp * rows + row] = square_send[0]
    total = jnp.broadcast_to(jnp.sum(square_recv[...], axis=0), (wanted_dev, LANES))
    column = grid_iota((wanted_dev, LANES), 0)
    unit = 1.0 / (SHIFT * SHIFT)
    ritz_squares, resid_squares = (
        jnp.sum(jnp.where(lane_dev == column + kind * wanted_dev, total, 0.0), axis=1, keepdims=True) * unit
        for kind in range(2)
    )
    ritz_squares = ritz_squares + 1.0
    factor_ref[...] = jnp.broadcast_to(
        jnp.sqrt(rows_total / ritz_squares) * (1.0 / SHIFT), (wanted_dev, LANES)
    )
    norms = jnp.broadcast_to(jnp.sqrt(resid_squares / ritz_squares), (wanted_dev, LANES))
    norm_ref[...] = jnp.sum(jnp.where(lane_dev == column, norms, 0.0), axis=0, keepdims=True)

    land(square_recv.at[pl.ds(0, others)], small_send.at[1])
    land(stat_send.at[pl.ds(1, groups - 1)], small_send.at[0])

    @pl.when(lead)
    def _():
        for kind, ref in enumerate((coefs, values)):
            land(ref, coef_send.at[kind])

    arrive(1, 1)
    arrive(3, 1)
    take((3, 1), pairs - 1, 0)
    land(coded, send_sem)


def finish_kernel(ritz_in, resid_in, factor_ref, norm_in, ritz_out, resid_out, norm_out, scaled, norm, sems):
    wanted_dev, _, inner = ritz_in.shape
    norm[...] = norm_in[0, :wanted_dev]
    norm_copy = pltpu.make_async_copy(norm, norm_out, sems.at[2])
    norm_copy.start()
    for column in range(wanted_dev):
        span = slice(column, column + 1)
        spot = jnp.broadcast_to(factor_ref[span], (TILE, LANES))
        spot = jnp.concatenate([spot] * (inner // LANES), axis=1)[None]
        for kind, (source, out) in enumerate(((ritz_in, ritz_out), (resid_in, resid_out))):
            for at in range(0, source.shape[1], TILE):
                scaled[kind, span, at : at + TILE] = source[span, at : at + TILE] * spot
            pltpu.make_async_copy(scaled.at[kind, span], out.at[span], sems.at[kind]).start()
    norm_copy.wait()
    for kind, out in enumerate((ritz_out, resid_out)):
        pltpu.make_async_copy(scaled.at[kind], out, sems.at[kind]).wait()


def body(groups, rows, krylov_basis, krylov_image, tridiag_vectors, ritz_values):
    krylov_len, outer_dev, inner_dev = krylov_basis.shape
    wanted_dev = tridiag_vectors.shape[1]
    chunks = outer_dev // TILE
    block = wanted_dev * TILE
    planes = rows // 2
    assert groups == 4 and rows == 2 * planes and chunks % 2 == 0
    padded_len = cdiv(krylov_len, STEP) * STEP
    rows_total = float(outer_dev * inner_dev * groups * rows)
    f32, bf16 = jnp.float32, jnp.bfloat16
    dma, regular = pltpu.SemaphoreType.DMA, pltpu.SemaphoreType.REGULAR
    vmem = pl.BlockSpec(memory_space=pltpu.VMEM)
    hbm = pl.BlockSpec(memory_space=pltpu.HBM)
    out = jax.ShapeDtypeStruct((wanted_dev, outer_dev, groups * inner_dev), f32)
    ritz, resid, factor, norms = pl.pallas_call(
        functools.partial(exchange_kernel, groups, rows, rows_total),
        name="exchange",
        out_shape=(
            out, out, jax.ShapeDtypeStruct((wanted_dev, LANES), f32), jax.ShapeDtypeStruct((1, LANES), f32),
        ),
        in_specs=[hbm] * 4,
        out_specs=(vmem,) * 4,
        scratch_shapes=[
            pltpu.VMEM((6, wanted_dev, krylov_len), bf16),
            pltpu.VMEM((6, 1, wanted_dev), bf16),
            pltpu.VMEM((chunks, 2, padded_len, TILE, inner_dev), bf16),
            pltpu.VMEM((LANES, LANES * TILE), bf16),
            pltpu.VMEM((2 * wanted_dev * TILE, padded_len * TILE), bf16),
            pltpu.VMEM((groups - 1, chunks, block, 2 * inner_dev), bf16),
            pltpu.VMEM((groups - 1, chunks, block, 2 * inner_dev), bf16),
            pltpu.VMEM((groups, wanted_dev, LANES), f32),
            pltpu.VMEM((groups, wanted_dev, LANES), f32),
            pltpu.VMEM((groups, 1, LANES), f32),
            pltpu.VMEM((groups * rows, 1, LANES), f32),
            dma((2,)),
            dma((2,)),
            dma((groups - 1, 2)),
            dma((2,)),
            dma,
            dma((groups - 1, 2)),
            dma((2,)),
            dma((3,)),
            regular,
            regular((2,)),
        ],
        compiler_params=pltpu.CompilerParams(
            collective_id=0, has_side_effects=True, vmem_limit_bytes=48 * MIB
        ),
    )(*[pltpu.with_memory_space_constraint(x, pltpu.HBM) for x in (tridiag_vectors.T, ritz_values[None])], krylov_basis, krylov_image)
    return pl.pallas_call(
        finish_kernel,
        name="finish",
        out_shape=(out, out, jax.ShapeDtypeStruct((wanted_dev,), f32)),
        in_specs=[vmem] * 4,
        out_specs=(hbm, hbm, hbm),
        scratch_shapes=[
            pltpu.VMEM((2, wanted_dev, outer_dev, groups * inner_dev), f32),
            pltpu.VMEM((wanted_dev,), f32),
            dma((3,)),
        ],
        compiler_params=pltpu.CompilerParams(vmem_limit_bytes=16 * MIB),
    )(ritz, resid, factor, norms)


def solution(mesh):
    placed = (P(None, "row", "grp"), P(None, "row", "grp"), P(None, "grp"), P("grp"))
    return jax.shard_map(
        functools.partial(body, mesh.shape["grp"], mesh.shape["row"]),
        mesh=mesh,
        in_specs=placed,
        out_specs=(P("grp", "row", None), P("grp", "row", None), P("grp")),
        check_vma=False,
    )
```

```python
import functools
import math

import jax
import jax.numpy as jnp
from jax import lax
from jax.experimental import pallas as pl
from jax.experimental.pallas import tpu as pltpu
from jax.sharding import PartitionSpec as P

MESH = pl.DeviceIdType.MESH
MIB = 1 << 20
TILE = 8
STEP = 16
LANES = 128
POWER = 13
PEAK = 2.0 ** (126.0 / POWER)
SHIFT = 2.0**30
LEAST = 1e-36


def cdiv(a, b):
    return (a + b - 1) // b


def grid_iota(shape, dim):
    return lax.broadcasted_iota(jnp.int32, shape, dim)


def expand_rows(cols, width):
    return jnp.broadcast_to(cols, (cols.shape[0], width)).reshape(cols.shape[0], 1, width)


def encode(cols, inverse):
    y = cols * inverse
    y2 = y * y
    y4 = y2 * y2
    y8 = y4 * y4
    return (y8 * y4) * y


def decode(codes):
    size = jnp.exp2(jnp.log(jnp.abs(codes)) * (1.0 / (POWER * math.log(2.0))))
    return jnp.where(codes < 0.0, -size, size)


def exchange_kernel(
    groups, rows, rows_total,
    tridiag_ref, values_ref, basis_ref, image_ref,
    ritz_ref, resid_ref, factor_ref, norm_ref,
    coefs, values, fields, spread, expanded, coded, received,
    stat_send, stat_recv, square_send, square_recv,
    coef_load, coef_send, coef_recv, load_sem, send_sem, recv_sem, small_send, small_recv,
    ready_sem, order_sem,
):
    wanted_dev, krylov_len = tridiag_ref.shape
    chunks = fields.shape[0]
    pairs = chunks // 2
    padded_len = fields.shape[2]
    inner_dev = basis_ref.shape[2]
    steps = padded_len // STEP
    wide = STEP * TILE
    block = wanted_dev * TILE
    planes = rows // 2
    grp = lax.axis_index("grp")
    row = lax.axis_index("row")
    core = lax.rem(row, 2)
    plane = lax.div(row, 2)
    lead = core == 1
    last_group = jnp.where(grp == groups - 1, 1, 0)

    def partner(mask):
        if mask == 0:
            return grp
        if mask == 1:
            return grp + 1 - 2 * lax.rem(grp, 2)
        if mask == 2:
            return lax.rem(grp + 2, groups)
        return groups - 1 - grp

    def device(mask, at_plane, at_core):
        return {"grp": partner(mask), "row": 2 * at_plane + at_core}

    def signal(sem, where):
        pl.semaphore_signal(sem, inc=1, device_id=where, device_id_type=MESH)

    barrier = pltpu.get_barrier_semaphore()
    for mask in (1, 2):
        signal(barrier, device(mask, plane, 1))

    coef_loads = [
        pltpu.make_async_copy(tridiag_ref, coefs.at[0], coef_load.at[0]),
        pltpu.make_async_copy(values_ref, values.at[0], coef_load.at[1]),
    ]
    for copy in coef_loads:
        copy.start()

    @pl.when(core == 0)
    def _():
        signal(barrier, device(0, plane, 1))

        def greet(ahead, carry):
            signal(barrier, device(0, lax.rem(plane + ahead, planes), 0))
            return carry

        lax.fori_loop(1, planes, greet, 0)

    for chunk in range(chunks):
        for which, ref in enumerate((basis_ref, image_ref)):
            pltpu.make_async_copy(
                ref.at[:, chunk * TILE : (chunk + 1) * TILE, :],
                fields.at[chunk, which, pl.ds(0, krylov_len)],
                load_sem.at[min(chunk // 2, 1)],
            ).start()

    def land(ref, sem):
        pltpu.make_async_copy(ref, ref, sem).wait()

    def load_wait(start, count):
        land(fields.at[pl.ds(start, count), :, pl.ds(0, krylov_len)], load_sem.at[min(start, 1)])

    if padded_len > krylov_len:
        for chunk in range(chunks):
            for which in range(2):
                fields[chunk, which, pl.ds(krylov_len, padded_len - krylov_len)] = jnp.zeros(
                    (padded_len - krylov_len, TILE, inner_dev), jnp.bfloat16
                )
    shape = spread.shape
    spread[...] = jnp.where(
        lax.shift_right_logical(grid_iota(shape, 1), 3) == grid_iota(shape, 0), SHIFT, 0.0
    ).astype(jnp.bfloat16)

    for copy in coef_loads:
        copy.wait()

    def coef_copies(source, slot, mask, at_core):
        return [
            pltpu.make_async_remote_copy(
                src_ref=ref.at[source],
                dst_ref=ref.at[slot],
                send_sem=coef_send.at[kind],
                recv_sem=coef_recv.at[slot - 1, kind],
                device_id=device(mask, plane, at_core),
                device_id_type=MESH,
            )
            for kind, ref in enumerate((coefs, values))
        ]

    own_sends = [
        copy
        for mask in (2, 1)
        for at_core in (0, 1)
        for copy in coef_copies(0, mask, mask, at_core)
    ]
    relay_sends = [copy for at_core in (1, 0) for copy in coef_copies(1, 3, 2, at_core)]

    def coef_wait(slot):
        for copy in coef_copies(0, slot, 1, 1):
            copy.wait_recv()

    @pl.when(lead)
    def _():
        pl.semaphore_wait(barrier, 5)
        for copy in own_sends:
            copy.start()
        signal(ready_sem, device(0, plane, 0))
        coef_wait(1)
        for copy in relay_sends:
            copy.start()
        coef_wait(2)

    @pl.when(core == 0)
    def _():
        pl.semaphore_wait(ready_sem, 1)
        coef_wait(1)
        coef_wait(2)

    near = grid_iota((wanted_dev, wanted_dev), 0) == grid_iota((wanted_dev, wanted_dev), 1)
    same = (grid_iota((TILE, wide), 1) & (TILE - 1)) == grid_iota((TILE, wide), 0)
    per_part = LANES // STEP
    pair = 2 * wanted_dev
    lane = grid_iota((pair, LANES), 1)

    def prepare(slots):
        shifts = []
        for slot in slots:
            spot = jnp.broadcast_to(values[slot].astype(jnp.float32), (wanted_dev, wanted_dev))
            shifts.append(jnp.sum(jnp.where(near, spot, 0.0), axis=1, keepdims=True))
        shift_values = expand_rows(jnp.concatenate(shifts, axis=0), inner_dev)
        both = jnp.concatenate([coefs[slot] for slot in slots], axis=0)
        for part in range(cdiv(krylov_len, LANES)):
            piece = both[:, part * LANES : min((part + 1) * LANES, krylov_len)]
            wider = jnp.dot(piece, spread[: piece.shape[1]], preferred_element_type=jnp.float32)
            for step in range(part * per_part, min((part + 1) * per_part, steps)):
                at = (step % per_part) * wide
                spot = jnp.where(same[None], wider[:, at : at + wide].reshape(pair, 1, wide), 0.0)
                expanded[:, step * wide : (step + 1) * wide] = spot.reshape(pair * TILE, wide).astype(jnp.bfloat16)
        return shift_values

    def compute(slots, shift_values, start, count, stats, after=None):
        both = jnp.concatenate(
            [
                fields[start + more, which].reshape(padded_len * TILE, inner_dev)
                for more in range(count)
                for which in range(2)
            ],
            axis=1,
        )
        product = jnp.dot(expanded[...], both, preferred_element_type=jnp.float32)
        product = product.reshape(pair, TILE, 2 * count * inner_dev)
        for more in range(count):
            chunk = start + more
            at = 2 * more * inner_dev
            ritz = product[:, :, at : at + inner_dev]
            resid = product[:, :, at + inner_dev : at + 2 * inner_dev] - shift_values * ritz
            for kind, cols in enumerate((ritz, resid)):
                squares = jnp.sum(jnp.sum(cols * cols, axis=1), axis=1, keepdims=True)
                stats = jnp.where(lane == 2 * chunk + kind, squares, stats)
                inverse = expand_rows(PEAK / jnp.sqrt(jnp.maximum(squares, LEAST)), inner_dev)
                for index, slot in enumerate(slots):
                    part = slice(index * wanted_dev, (index + 1) * wanted_dev)
                    if slot == 0:
                        put_out(kind, chunk, grp, cols[part])
                    else:
                        coded[slot - 1, chunk, :, kind * inner_dev : (kind + 1) * inner_dev] = encode(
                            cols[part], inverse[part]
                        ).reshape(block, inner_dev).astype(jnp.bfloat16)
            if after is not None:
                after(chunk)
        return stats

    def put_out(kind, chunk, source, cols):
        span = pl.ds(pl.multiple_of(chunk * TILE, TILE), TILE)
        lanes = pl.ds(pl.multiple_of(source * inner_dev, inner_dev), inner_dev)
        (ritz_ref, resid_ref)[kind][:, span, lanes] = cols

    def data_copy(mask, start, final=0, count=2):
        span = pl.ds(start, count)
        return pltpu.make_async_remote_copy(
            src_ref=coded.at[mask - 1, span],
            dst_ref=received.at[mask - 1, span],
            send_sem=send_sem,
            recv_sem=recv_sem.at[mask - 1, final],
            device_id=device(mask, plane, core),
            device_id_type=MESH,
        )

    def stat_copy(mask):
        return pltpu.make_async_remote_copy(
            src_ref=stat_send.at[mask],
            dst_ref=stat_recv.at[mask],
            send_sem=small_send.at[0],
            recv_sem=small_recv.at[0 if mask < 3 else 2],
            device_id=device(mask, plane, core),
            device_id_type=MESH,
        )

    def squares_to(mask, at_plane, flip):
        pltpu.make_async_remote_copy(
            src_ref=square_send.at[mask],
            dst_ref=square_recv.at[grp * rows + row],
            send_sem=small_send.at[1],
            recv_sem=small_recv.at[1],
            device_id=device(mask, at_plane, lax.rem(core + flip, 2)),
            device_id_type=MESH,
        ).start()

    def far_squares(at_plane, carry):
        for mask in range(groups):
            for flip in range(2):
                squares_to(mask, at_plane, flip)
        return carry

    def agree(side, count):
        @pl.when(core == 0)
        def _():
            pl.semaphore_wait(order_sem.at[side], count)
            signal(order_sem.at[side], device(0, plane, 1))

        @pl.when(lead)
        def _():
            pl.semaphore_wait(order_sem.at[side], 1)

    def finish_stats(slots, stats):
        parity = lane & 1
        column = lax.rem(grid_iota((pair, LANES), 0), wanted_dev)
        line = jnp.zeros((pair, LANES), jnp.float32)
        for kind in range(2):
            sums = jnp.sum(jnp.where(parity == kind, stats, 0.0), axis=1, keepdims=True)
            line = jnp.where(lane == column + kind * wanted_dev, sums, line)
        scales = jnp.sqrt(jnp.maximum(stats, LEAST))
        for index, slot in enumerate(slots):
            part = slice(index * wanted_dev, (index + 1) * wanted_dev)
            square_send[slot] = jnp.sum(line[part], axis=0, keepdims=True)
            if slot:
                stat_send[slot] = scales[part]

    nothing = jnp.zeros((pair, LANES), jnp.float32)
    load_wait(0, 2)
    shift_values = prepare((1, 2))

    def send_chunk(chunk):
        for mask in (2, 1):
            data_copy(mask, chunk, count=1).start()

    stats = compute((1, 2), shift_values, 0, 2, nothing, send_chunk)
    load_wait(2, chunks - 2)
    def first(step, stats):
        stats = compute((1, 2), shift_values, 2 * step, 2, stats)
        @pl.when(step < pairs - 1)
        def _():
            data_copy(2, 2 * step).start()

        @pl.when(step < pairs - 1 - last_group)
        def _():
            data_copy(1, 2 * step).start()

        return stats

    stats = lax.fori_loop(1, pairs, first, stats)
    finish_stats((1, 2), stats)
    for mask in (2, 1):
        stat_copy(mask).start()

    @pl.when(core == 0)
    def _():
        data_copy(2, chunks - 2, 1).start()


    coef_wait(3)
    if planes > 1:
        @pl.when(core == 0)
        def _():
            pl.semaphore_wait(barrier, planes - 1)

            def lower(other, carry):
                signal(order_sem.at[1], device(0, other, 0))
                return carry

            def upper(other, carry):
                signal(order_sem.at[0], device(0, other, 0))
                return carry

            lax.fori_loop(plane + 1, planes, upper, 0)
            lax.fori_loop(0, plane, lower, 0)

    shift_other = prepare((3, 0))

    def second(step, stats):
        stats = compute((3, 0), shift_other, 2 * step, 2, stats)

        @pl.when(jnp.logical_and(last_group == 0, lax.rem(step, 2) == 0))
        def _():
            data_copy(3, step).start()

        @pl.when(jnp.logical_and(last_group == 1, step < pairs - 1))
        def _():
            data_copy(3, 2 * step).start()

        return stats

    stats = lax.fori_loop(0, pairs, second, nothing)
    finish_stats((3, 0), stats)

    stat_copy(3).start()
    for mask in range(groups):
        for flip in range(0 if mask else 1, 2):
            squares_to(mask, plane, flip)
    if planes > 1:
        @pl.when(plane > 0)
        def _():
            agree(0, plane)
            lax.fori_loop(0, plane, far_squares, 0)

    def across(step, carry):
        data_copy(3, 2 * step).start()
        return carry

    lax.fori_loop(jnp.where(last_group == 1, pairs - 1, cdiv(pairs, 2)), pairs - 1, across, 0)
    data_copy(3, chunks - 2, 1).start()

    @pl.when(last_group == 1)
    def _():
        data_copy(1, chunks - 4).start()


    @pl.when(core == 0)
    def _():
        data_copy(1, chunks - 2, 1).start()


    if planes > 1:
        @pl.when(plane < planes - 1)
        def _():
            agree(1, planes - 1 - plane)
            lax.fori_loop(plane + 1, planes, far_squares, 0)

    @pl.when(lead)
    def _():
        data_copy(2, chunks - 2, 1).start()
        data_copy(1, chunks - 2, 1).start()

    land(stat_recv.at[pl.ds(1, 2)], small_recv.at[0])

    lane_dev = grid_iota((wanted_dev, LANES), 1)

    def arrive(mask, final):
        span = pl.ds(chunks - 2, 2) if final else pl.ds(0, chunks - 2)
        land(received.at[mask - 1, span], recv_sem.at[mask - 1, final])

    def take(masks, step, carry):
        for half in range(2):
            chunk = 2 * step + half
            for mask in masks:
                for kind in range(2):
                    scale = jnp.sum(
                        jnp.where(lane_dev == 2 * chunk + kind, stat_recv[mask], 0.0), axis=1, keepdims=True
                    )
                    codes = received[mask - 1, chunk, :, kind * inner_dev : (kind + 1) * inner_dev]
                    size = decode(codes.astype(jnp.float32)).reshape(wanted_dev, TILE, inner_dev)
                    put_out(kind, chunk, partner(mask), size * expand_rows(scale * (1.0 / PEAK), inner_dev))
        return carry

    arrive(2, 0)

    arrive(1, 0)
    lax.fori_loop(0, pairs - 1, functools.partial(take, (1, 2)), 0)
    land(stat_recv.at[3], small_recv.at[2])
    arrive(3, 0)
    lax.fori_loop(0, pairs - 1, functools.partial(take, (3,)), 0)
    arrive(2, 1)
    take((2,), pairs - 1, 0)

    others = groups * rows - 1
    land(square_recv.at[pl.ds(0, others)], small_recv.at[1])
    square_recv[grp * rows + row] = square_send[0]
    total = jnp.broadcast_to(jnp.sum(square_recv[...], axis=0), (wanted_dev, LANES))
    column = grid_iota((wanted_dev, LANES), 0)
    unit = 1.0 / (SHIFT * SHIFT)
    ritz_squares, resid_squares = (
        jnp.sum(jnp.where(lane_dev == column + kind * wanted_dev, total, 0.0), axis=1, keepdims=True) * unit
        for kind in range(2)
    )
    ritz_squares = ritz_squares + 1.0
    factor_ref[...] = jnp.broadcast_to(
        jnp.sqrt(rows_total / ritz_squares) * (1.0 / SHIFT), (wanted_dev, LANES)
    )
    norms = jnp.broadcast_to(jnp.sqrt(resid_squares / ritz_squares), (wanted_dev, LANES))
    norm_ref[...] = jnp.sum(jnp.where(lane_dev == column, norms, 0.0), axis=0, keepdims=True)

    land(square_recv.at[pl.ds(0, others)], small_send.at[1])
    land(stat_send.at[pl.ds(1, groups - 1)], small_send.at[0])

    @pl.when(lead)
    def _():
        for kind, ref in enumerate((coefs, values)):
            land(ref, coef_send.at[kind])

    arrive(1, 1)
    arrive(3, 1)
    take((3, 1), pairs - 1, 0)
    land(coded, send_sem)


def finish_kernel(ritz_in, resid_in, factor_ref, norm_in, ritz_out, resid_out, norm_out, scaled, norm, sems):
    wanted_dev, _, inner = ritz_in.shape
    norm[...] = norm_in[0, :wanted_dev]
    norm_copy = pltpu.make_async_copy(norm, norm_out, sems.at[2])
    norm_copy.start()
    for column in range(wanted_dev):
        span = slice(column, column + 1)
        spot = jnp.broadcast_to(factor_ref[span], (TILE, LANES))
        spot = jnp.concatenate([spot] * (inner // LANES), axis=1)[None]
        for kind, (source, out) in enumerate(((ritz_in, ritz_out), (resid_in, resid_out))):
            for at in range(0, source.shape[1], TILE):
                scaled[kind, span, at : at + TILE] = source[span, at : at + TILE] * spot
            pltpu.make_async_copy(scaled.at[kind, span], out.at[span], sems.at[kind]).start()
    norm_copy.wait()
    for kind, out in enumerate((ritz_out, resid_out)):
        pltpu.make_async_copy(scaled.at[kind], out, sems.at[kind]).wait()


def body(groups, rows, krylov_basis, krylov_image, tridiag_vectors, ritz_values):
    krylov_len, outer_dev, inner_dev = krylov_basis.shape
    wanted_dev = tridiag_vectors.shape[1]
    chunks = outer_dev // TILE
    block = wanted_dev * TILE
    planes = rows // 2
    assert groups == 4 and rows == 2 * planes and chunks % 2 == 0
    padded_len = cdiv(krylov_len, STEP) * STEP
    rows_total = float(outer_dev * inner_dev * groups * rows)
    f32, bf16 = jnp.float32, jnp.bfloat16
    dma, regular = pltpu.SemaphoreType.DMA, pltpu.SemaphoreType.REGULAR
    vmem = pl.BlockSpec(memory_space=pltpu.VMEM)
    hbm = pl.BlockSpec(memory_space=pltpu.HBM)
    out = jax.ShapeDtypeStruct((wanted_dev, outer_dev, groups * inner_dev), f32)
    ritz, resid, factor, norms = pl.pallas_call(
        functools.partial(exchange_kernel, groups, rows, rows_total),
        name="exchange",
        out_shape=(
            out, out, jax.ShapeDtypeStruct((wanted_dev, LANES), f32), jax.ShapeDtypeStruct((1, LANES), f32),
        ),
        in_specs=[hbm] * 4,
        out_specs=(vmem,) * 4,
        scratch_shapes=[
            pltpu.VMEM((6, wanted_dev, krylov_len), bf16),
            pltpu.VMEM((6, 1, wanted_dev), bf16),
            pltpu.VMEM((chunks, 2, padded_len, TILE, inner_dev), bf16),
            pltpu.VMEM((LANES, LANES * TILE), bf16),
            pltpu.VMEM((2 * wanted_dev * TILE, padded_len * TILE), bf16),
            pltpu.VMEM((groups - 1, chunks, block, 2 * inner_dev), bf16),
            pltpu.VMEM((groups - 1, chunks, block, 2 * inner_dev), bf16),
            pltpu.VMEM((groups, wanted_dev, LANES), f32),
            pltpu.VMEM((groups, wanted_dev, LANES), f32),
            pltpu.VMEM((groups, 1, LANES), f32),
            pltpu.VMEM((groups * rows, 1, LANES), f32),
            dma((2,)),
            dma((2,)),
            dma((groups - 1, 2)),
            dma((2,)),
            dma,
            dma((groups - 1, 2)),
            dma((2,)),
            dma((3,)),
            regular,
            regular((2,)),
        ],
        compiler_params=pltpu.CompilerParams(
            collective_id=0, has_side_effects=True, vmem_limit_bytes=48 * MIB
        ),
    )(*[pltpu.with_memory_space_constraint(x, pltpu.HBM) for x in (tridiag_vectors.T, ritz_values[None])], krylov_basis, krylov_image)
    return pl.pallas_call(
        finish_kernel,
        name="finish",
        out_shape=(out, out, jax.ShapeDtypeStruct((wanted_dev,), f32)),
        in_specs=[vmem] * 4,
        out_specs=(hbm, hbm, hbm),
        scratch_shapes=[
            pltpu.VMEM((2, wanted_dev, outer_dev, groups * inner_dev), f32),
            pltpu.VMEM((wanted_dev,), f32),
            dma((3,)),
        ],
        compiler_params=pltpu.CompilerParams(vmem_limit_bytes=16 * MIB),
    )(ritz, resid, factor, norms)


def solution(mesh):
    placed = (P(None, "row", "grp"), P(None, "row", "grp"), P(None, "grp"), P("grp"))
    return jax.shard_map(
        functools.partial(body, mesh.shape["grp"], mesh.shape["row"]),
        mesh=mesh,
        in_specs=placed,
        out_specs=(P("grp", "row", None), P("grp", "row", None), P("grp")),
        check_vma=False,
    )
```
